32 devices in a mesh: aux: 8 (over z, x), lmo: 4 (over y, core).
Axes of the slice: x: 2, y: 2, z: 4, core: 2. Of those that a mesh axis runs over, the one named last changes fastest.
Arguments:
- aux_ints: bfloat16 [256, 768, 768], P(('aux', 'lmo')), may hold values from -6 to 6
- lmo_coef: bfloat16 [128, 384], P(('aux', 'lmo')), may hold values from -0.3125 to 0.3125
- ao_domain: int32 [128, 3], replicated, may hold values from 0 to 5, as said below
- ao_count: int32 [128], replicated, may hold values from 1 to 3
- pao_domain: int32 [128, 3], replicated, may hold values from 0 to 5, as said below
- pao_count: int32 [128], replicated, may hold values from 1 to 3, as said below
- owner_order: int32 [128], replicated, may hold values from 0 to 127, as said below
- pao_coef: bfloat16 [128, 384, 256], P(('aux', 'lmo')), may hold values from -0.3125 to 0.3125
Outputs:
- pair_ints: bfloat16 [128, 256, 256], P(('aux', 'lmo'))
- pair_metric: float32 [128, 256, 256], P(('aux', 'lmo'))
The draws below stay inside these ranges and needn't reach their ends.
Inputs may be any that keep to these rules, and one draw needn't show every extreme that they name: `ao_domain`: each row holds 3 different block numbers; slots from ao_count on are unused. `pao_domain`: each row holds 3 different block numbers; slots from pao_count on are unused. `pao_count`: the LMOs of the 4 owner slots of one device use together at most 8 PAO block slots, and those of some device use exactly 8. `owner_order`: every LMO stands in exactly one slot.
All inputs are finite; a program needn't handle non-finite values.
Results may differ from the reference program's by a relative error of at most 0.0049.
Values may be sent and summed in bfloat16 or wider, within the bound.
A program may use at most 128 MiB of HBM per device.

```python
import jax
import jax.numpy as jnp
from jax import lax

BLK = 128
NBA = 6
DB = 3
PB = 3
NPAO = 256
P_D = 8
LMO_DEV = 4
AO = 768
NAUX = 256
NLMO = 128
USED = 8


def draw_rows(key, row_depth):
    subkeys = jax.random.split(key, NLMO)

    def one_row(subkey):
        return jax.random.permutation(subkey, NBA)[:row_depth]
    return jax.vmap(one_row)(subkeys).astype(jnp.int32)


def draw_ao_domain(key, part):
    return draw_rows(jax.random.fold_in(key, 11), DB)


def draw_pao_domain(key, part):
    return draw_rows(jax.random.fold_in(key, 23), PB)


def owner_tables(key):
    base = jax.random.fold_in(key, 31)
    order_key, target_key, full_key, unit_key = jax.random.split(base, 4)
    order = jax.random.permutation(order_key, NLMO).astype(jnp.int32)
    groups = NLMO // LMO_DEV
    target = jax.random.randint(target_key, (groups,), LMO_DEV, USED + 1).astype(jnp.int32)
    full_group = jax.random.randint(full_key, (), 0, groups).astype(jnp.int32)
    target = jnp.where(jnp.arange(groups, dtype=jnp.int32) == full_group, USED, target)
    counts = jnp.ones((groups, LMO_DEV), jnp.int32)
    members = jnp.arange(LMO_DEV, dtype=jnp.int32)
    for unit in range(USED - LMO_DEV):
        scores = jax.random.randint(jax.random.fold_in(unit_key, unit), (groups, LMO_DEV), 0, 1 << 20).astype(jnp.int32)
        scores = scores * LMO_DEV + members[None, :]
        scores = jnp.where(counts < PB, scores, -1)
        picked = jnp.argmax(scores, axis=1).astype(jnp.int32)
        adding = (members[None, :] == picked[:, None]) & (unit < target - LMO_DEV)[:, None]
        counts = counts + adding.astype(jnp.int32)
    by_slot = counts.reshape(NLMO)
    pao_count = jnp.zeros((NLMO,), jnp.int32).at[order].set(by_slot)
    return (order, pao_count)


def draw_owner_order(key, part):
    return owner_tables(key)[0]


def draw_pao_count(key, part):
    return owner_tables(key)[1]


def set_ends(entries, stream_key, low, high):
    longest = entries.shape.index(max(entries.shape))
    spots = []
    for shift in (0, 1):
        where = [jax.random.randint(jax.random.fold_in(stream_key, axis), (), 0, length) for axis, length in enumerate(entries.shape)]
        where[longest] = (where[longest] + shift) % entries.shape[longest]
        spots.append(tuple(where))
    return entries.at[spots[0]].set(low).at[spots[1]].set(high)


def shard_levels(stream_key, shape, shards, least, high):
    factor_of, own = 1.0, jax.random.fold_in(stream_key, 6)
    for position, shards_of in shards:
        steps = jnp.exp(jax.random.uniform(jax.random.fold_in(own, position), (shards_of,), jnp.float32, least / len(shards), high / len(shards)))
        factor_of = factor_of * jnp.repeat(steps, shape[position] // shards_of).reshape([-1 if axis == position else 1 for axis in range(len(shape))])
    return factor_of


def gaussian(stream_key, dims, spread, reach, cuts=(), kind=jnp.bfloat16):
    values = jax.random.normal(stream_key, dims, jnp.float32) * spread
    if len(cuts) > 0:
        values = shard_levels(stream_key, dims, cuts, -0.22, 0.18) * values
    return jnp.clip(values, min=-reach, max=reach).astype(kind)


def setup_inputs(seed: int = 0) -> dict:
    streams_of = jax.random.split(jax.random.key(seed), 9)
    aux_ints = gaussian(streams_of[0], (NAUX, AO, AO), 1.0, 6.0, ((0, 32),))
    lmo_coef = gaussian(streams_of[1], (NLMO, DB * BLK), (DB * BLK) ** -0.5, 0.3125, ((0, 32),))
    ao_domain = draw_ao_domain(jax.random.fold_in(streams_of[8], 71), 0)
    ao_count = set_ends(jax.random.randint(streams_of[3], (NLMO,), 1, DB + 1), jax.random.fold_in(streams_of[3], 1), 1, DB).astype(jnp.int32)
    pao_domain = draw_pao_domain(jax.random.fold_in(streams_of[8], 71), 0)
    pao_count = draw_pao_count(jax.random.fold_in(streams_of[8], 71), 0)
    owner_order = draw_owner_order(jax.random.fold_in(streams_of[8], 71), 0)
    pao_coef = gaussian(streams_of[7], (NLMO, PB * BLK, NPAO), (PB * BLK) ** -0.5, 0.3125, ((0, 32),))
    return dict(aux_ints=aux_ints, lmo_coef=lmo_coef, ao_domain=ao_domain, ao_count=ao_count, pao_domain=pao_domain, pao_count=pao_count, owner_order=owner_order, pao_coef=pao_coef)


def place(lmo_coef, domain, block_count, blocks):
    lmo_total = lmo_coef.shape[0]
    in_domain = jnp.arange(DB)[None, :] < block_count[:, None]
    onehot = ((domain[:, :, None] == jnp.arange(blocks)[None, None, :]) & in_domain[:, :, None]).astype(jnp.float32)
    tiles = lmo_coef.astype(jnp.float32).reshape(lmo_total, DB, BLK)
    dense_coef = jnp.einsum("ikb,ikn->bni", onehot, tiles, precision=lax.Precision.HIGHEST)
    return dense_coef.reshape(blocks * BLK, lmo_total).astype(jnp.bfloat16)


def select(half_ints, domain, block_count, blocks):
    row_total = half_ints.shape[0]
    lmo_total = half_ints.shape[2]
    in_domain = jnp.arange(PB)[None, :] < block_count[:, None]
    onehot = ((domain[:, :, None] == jnp.arange(blocks)[None, None, :]) & in_domain[:, :, None]).astype(jnp.float32)
    tiled = half_ints.reshape(row_total, blocks, BLK, lmo_total)
    picked = jnp.einsum("pbni,ikb->ipkn", tiled, onehot, precision=lax.Precision.HIGHEST)
    return picked.reshape(lmo_total, row_total, PB * BLK).astype(jnp.bfloat16)


def reference(aux_ints, lmo_coef, ao_domain, ao_count, pao_domain, pao_count, owner_order, pao_coef):
    blocks = aux_ints.shape[1] // BLK
    dense_coef = place(lmo_coef, ao_domain, ao_count, blocks)

    def transform(block_ints):
        row_total = block_ints.shape[0]
        half_ints = jnp.dot(block_ints.reshape(row_total * AO, AO), dense_coef,
                            preferred_element_type=jnp.float32).reshape(row_total, AO, -1)
        return select(half_ints, pao_domain, pao_count, blocks)

    stacked = lax.map(transform, aux_ints.reshape(NAUX // P_D, P_D, AO, AO))
    selected = jnp.transpose(stacked, (1, 0, 2, 3)).reshape(NLMO, NAUX, PB * BLK)
    ordered = selected[owner_order]

    def per_slot(operands):
        rows_here, coef_here = operands
        pair_row = jnp.dot(rows_here, coef_here, preferred_element_type=jnp.float32).astype(jnp.bfloat16)
        wide_row = pair_row.astype(jnp.float32)
        metric_row = jnp.dot(wide_row.T, wide_row, precision=lax.Precision.HIGHEST) / NAUX
        return pair_row, metric_row

    pair_ints, pair_metric = lax.map(per_slot, (ordered, pao_coef))
    return pair_ints, pair_metric
```

```python
import functools

import jax
import jax.numpy as jnp
from jax import lax
from jax.experimental import pallas as pl
from jax.experimental.pallas import tpu as pltpu
from jax.sharding import PartitionSpec as P

BLK = 128
DB = 3
PB = 3
USED = 8
MESH = pl.DeviceIdType.MESH


def exchange(
    n_aux, n_lmo, plane,
    aux_hbm, lmo_hbm, ao_dom_hbm, ao_cnt_hbm, pao_dom_hbm, pao_cnt_hbm, order_hbm, recv,
    aux, aux_t, lmo_ref, ao_dom, ao_cnt, pao_dom, pao_cnt, order,
    coef_all, coef32, dense, half, tab, send,
    aux_sem, in_sem, entered, coef_send, coef_recv, out_send, out_recv,
):
    dev = n_aux * n_lmo
    rows, ao, _ = aux_hbm.shape
    blocks = ao // BLK
    per = lmo_hbm.shape[0]
    lmos = per * dev
    planes = dev // plane
    me = lax.axis_index("aux") * n_lmo + lax.axis_index("lmo")
    my_plane, seat = me // plane, lax.rem(me, plane)

    def coords(d):
        return (d // n_lmo, lax.rem(d, n_lmo))

    barrier = pltpu.get_barrier_semaphore()

    @pl.loop(me + 1, dev)
    def _(d):
        pl.semaphore_signal(barrier, inc=1, device_id=coords(d), device_id_type=MESH)

    small = [
        pltpu.make_async_copy(src, dst, in_sem.at[n])
        for n, (src, dst) in enumerate((
            (lmo_hbm, lmo_ref), (ao_dom_hbm, ao_dom), (ao_cnt_hbm, ao_cnt),
            (pao_dom_hbm, pao_dom), (pao_cnt_hbm, pao_cnt), (order_hbm, order),
        ))
    ]
    for copy in small:
        copy.start()

    def load(p):
        return pltpu.make_async_copy(aux_hbm.at[p], aux.at[p], aux_sem.at[p])

    for p in range(rows):
        load(p).start()

    def coef_copy(slot, d):
        return pltpu.make_async_remote_copy(
            src_ref=lmo_ref, dst_ref=coef_all.at[slot],
            send_sem=coef_send.at[d], recv_sem=coef_recv.at[slot],
            device_id=coords(d), device_id_type=MESH,
        )

    @pl.when(me > 0)
    def _():
        pl.semaphore_wait(barrier, me)

    @pl.loop(0, me)
    def _(d):
        pl.semaphore_signal(entered.at[me], inc=1, device_id=coords(d), device_id_type=MESH)

    small[0].wait()

    @pl.loop(0, me)
    def _(d):
        coef_copy(me, d).start()

    coef_all[me] = lmo_ref[...]
    for copy in small[1:]:
        copy.wait()

    def greet(first, last):
        @pl.loop(first, last)
        def _(d):
            pl.semaphore_wait(entered.at[d], 1)
            coef_copy(me, d).start()

    @pl.loop(0, dev)
    def _(d):
        lmo = [order[d * per + j] for j in range(per)]
        cnt = [pao_cnt[i] for i in lmo]
        for s in range(USED):
            i, k = lmo[0], jnp.int32(s)
            start = jnp.int32(0)
            for j in range(1, per):
                start = start + cnt[j - 1]
                past = s >= start
                i = jnp.where(past, lmo[j], i)
                k = jnp.where(past, s - start, k)
            tab[d * USED + s] = i * blocks + pao_dom[jnp.minimum(k, PB - 1), i]

    eye = lax.broadcasted_iota(jnp.int32, (lmos, lmos), 0) == lax.broadcasted_iota(
        jnp.int32, (lmos, lmos), 1
    )
    where_to = []
    for k in range(DB):
        block = jnp.where(ao_cnt[...] > k, ao_dom[k:k + 1, :], -1).astype(jnp.float32)
        column = jnp.sum(jnp.where(eye, block, 0.0), axis=1, keepdims=True)
        where_to.append(jnp.broadcast_to(column, (lmos, BLK)))

    later = dev - 1 - me
    for p in range(rows):
        load(p).wait()
        aux_t[p] = aux[p].T
        greet(me + 1 + later * p // rows, me + 1 + later * (p + 1) // rows)

    @pl.loop(0, me)
    def _(d):
        coef_copy(d, d).wait_recv()

    @pl.loop(me + 1, dev)
    def _(d):
        coef_copy(d, d).wait_recv()

    for d in range(dev):
        coef32[d * per:(d + 1) * per, :] = coef_all[d].astype(jnp.float32)
    for b in range(blocks):
        total = jnp.zeros((lmos, BLK), jnp.float32)
        for k in range(DB):
            total = jnp.where(where_to[k] == b, coef32[:, k * BLK:(k + 1) * BLK], total)
        dense[:, b * BLK:(b + 1) * BLK] = total.astype(jnp.bfloat16)

    flat = half.reshape(lmos * blocks * rows, BLK)
    wide = 2
    for p in range(rows):
        for b in range(0, blocks, wide):
            out = jnp.dot(
                dense[...], aux_t[p, :, b * BLK:(b + wide) * BLK],
                preferred_element_type=jnp.float32,
            )
            for c in range(wide):
                flat[pl.ds((b + c) * rows + p, lmos, stride=blocks * rows), :] = (
                    out[:, c * BLK:(c + 1) * BLK]
                )

    def packed(d, s):
        return half[tab[d * USED + s]].astype(jnp.bfloat16)

    def pack(d):
        for s in range(USED):
            send[d, s] = packed(d, s)

    def out_copy(slot, d):
        return pltpu.make_async_remote_copy(
            src_ref=send.at[d], dst_ref=recv.at[slot],
            send_sem=out_send.at[d], recv_sem=out_recv.at[slot],
            device_id=coords(d), device_id_type=MESH,
        )

    def target(t):
        i, j = t // plane, lax.rem(t, plane)
        own = i == planes - 1
        other = jnp.where(i >= my_plane, i + 1, i)
        return jnp.where(
            own,
            my_plane * plane + lax.rem(seat + 1 + j, plane),
            other * plane + lax.rem(seat + j, plane),
        )

    pack(target(0))

    @pl.loop(0, dev - 2)
    def _(t):
        pack(target(t + 1))
        out_copy(me, target(t)).start()

    for s in range(USED):
        recv[me, s] = packed(me, s)
    out_copy(me, target(dev - 2)).start()

    @pl.loop(0, dev - 1)
    def _(t):
        d = target(t)
        coef_copy(d, d).wait_send()
        out_copy(d, d).wait_send()

    @pl.loop(0, dev - 1)
    def _(t):
        d = target(t)
        out_copy(d, d).wait_recv()


def contract(n_lmo, per, recv, coef, pao_cnt, order, pair, metric, pair_out, metric_out, sem):
    me = lax.axis_index("aux") * n_lmo + lax.axis_index("lmo")
    dev, _, rows, _ = recv.shape
    start = jnp.int32(0)
    copies = []
    for g in range(per):
        count = pao_cnt[order[me * per + g]]
        tiles = []
        for k in range(PB):
            slot = jnp.minimum(start + k, USED - 1)
            tile = recv[:, slot].astype(jnp.float32).reshape(dev * rows, BLK)
            tiles.append(jnp.where(k < count, tile, 0.0).astype(jnp.bfloat16))
        start = start + count
        row = jnp.dot(
            jnp.concatenate(tiles, axis=1), coef[g], preferred_element_type=jnp.float32
        ).astype(jnp.bfloat16)
        pair_out[g] = row
        metric_out[g] = lax.dot_general(
            row, row, (((0,), (0,)), ((), ())), preferred_element_type=jnp.float32
        ) / (dev * rows)
        for c, (src, dst) in enumerate(((pair_out, pair), (metric_out, metric))):
            copies.append(pltpu.make_async_copy(src.at[g], dst.at[g], sem.at[g, c]))
            copies[-1].start()
    for copy in copies:
        copy.wait()


def shards(mesh, aux_ints, lmo_coef, ao_domain, ao_count, pao_domain, pao_count, owner_order, pao_coef):
    n_aux, n_lmo = mesh.shape["aux"], mesh.shape["lmo"]
    dev = n_aux * n_lmo
    rows, ao, _ = aux_ints.shape
    blocks = ao // BLK
    per = lmo_coef.shape[0]
    lmos = per * dev
    npao = pao_coef.shape[2]
    across = n_lmo // 2 if n_lmo % 2 == 0 and n_aux % (n_lmo // 2) == 0 else 1
    plane = across * n_lmo
    vmem = pl.BlockSpec(memory_space=pltpu.VMEM)
    smem = pl.BlockSpec(memory_space=pltpu.SMEM)
    anywhere = pl.BlockSpec(memory_space=pl.ANY)
    recv = pl.pallas_call(
        functools.partial(exchange, n_aux, n_lmo, plane),
        out_shape=pltpu.VMEM((dev, USED, rows, BLK), jnp.bfloat16),
        in_specs=[anywhere] * 7,
        out_specs=vmem,
        scratch_shapes=[
            pltpu.VMEM((rows, ao, ao), jnp.bfloat16),
            pltpu.VMEM((rows, ao, ao), jnp.bfloat16),
            pltpu.VMEM((per, DB * BLK), jnp.bfloat16),
            pltpu.VMEM((DB, lmos), jnp.int32),
            pltpu.VMEM((1, lmos), jnp.int32),
            pltpu.SMEM((PB, lmos), jnp.int32),
            pltpu.SMEM((lmos,), jnp.int32),
            pltpu.SMEM((lmos,), jnp.int32),
            pltpu.VMEM((dev, per, DB * BLK), jnp.bfloat16),
            pltpu.VMEM((lmos, DB * BLK), jnp.float32),
            pltpu.VMEM((lmos, ao), jnp.bfloat16),
            pltpu.VMEM((lmos * blocks, rows, BLK), jnp.float32),
            pltpu.SMEM((dev * USED,), jnp.int32),
            pltpu.VMEM((dev, USED, rows, BLK), jnp.bfloat16),
            pltpu.SemaphoreType.DMA((rows,)),
            pltpu.SemaphoreType.DMA((6,)),
            pltpu.SemaphoreType.REGULAR((dev,)),
            pltpu.SemaphoreType.DMA((dev,)),
            pltpu.SemaphoreType.DMA((dev,)),
            pltpu.SemaphoreType.DMA((dev,)),
            pltpu.SemaphoreType.DMA((dev,)),
        ],
        compiler_params=pltpu.CompilerParams(
            collective_id=0, has_side_effects=True, vmem_limit_bytes=48 * 2**20
        ),
        name="exchange",
    )(*(
        pltpu.with_memory_space_constraint(x, pltpu.HBM)
        for x in (aux_ints, lmo_coef, ao_domain.T, ao_count.reshape(1, lmos), pao_domain.T, pao_count, owner_order)
    ))
    pair, metric = pl.pallas_call(
        functools.partial(contract, n_lmo, per),
        out_shape=(
            jax.ShapeDtypeStruct((per, dev * rows, npao), jnp.bfloat16),
            jax.ShapeDtypeStruct((per, npao, npao), jnp.float32),
        ),
        in_specs=[vmem, vmem, smem, smem],
        out_specs=(anywhere, anywhere),
        scratch_shapes=[
            pltpu.VMEM((per, dev * rows, npao), jnp.bfloat16),
            pltpu.VMEM((per, npao, npao), jnp.float32),
            pltpu.SemaphoreType.DMA((per, 2)),
        ],
        compiler_params=pltpu.CompilerParams(vmem_limit_bytes=24 * 2**20),
        name="contract",
    )(recv, pao_coef, pao_count, owner_order)
    return pair, metric


def solution(mesh):
    split = ("aux", "lmo")
    placed = (P(split, None, None), P(split, None), P(), P(), P(), P(), P(), P(split, None, None))
    return jax.shard_map(
        functools.partial(shards, mesh),
        mesh=mesh,
        in_specs=placed,
        out_specs=(P(split, None, None), P(split, None, None)),
        check_vma=False,
    )
```

```python
import functools

import jax
import jax.numpy as jnp
from jax import lax
from jax.experimental import pallas as pl
from jax.experimental.pallas import tpu as pltpu
from jax.sharding import PartitionSpec as P

BLK = 128
DB = 3
PB = 3
USED = 8
MESH = pl.DeviceIdType.MESH


def exchange(
    n_aux, n_lmo, plane,
    aux_hbm, lmo_hbm, ao_dom_hbm, ao_cnt_hbm, pao_dom_hbm, pao_cnt_hbm, order_hbm, recv,
    aux, aux_t, lmo_ref, ao_dom, ao_cnt, pao_dom, pao_cnt, order,
    coef_all, coef32, dense, half, send,
    aux_sem, in_sem, entered, coef_send, coef_recv, out_send, out_recv,
):
    dev = n_aux * n_lmo
    rows, ao, _ = aux_hbm.shape
    blocks = ao // BLK
    per = lmo_hbm.shape[0]
    lmos = per * dev
    planes = dev // plane
    me = lax.axis_index("aux") * n_lmo + lax.axis_index("lmo")
    my_plane, seat = me // plane, lax.rem(me, plane)

    def coords(d):
        return (d // n_lmo, lax.rem(d, n_lmo))

    barrier = pltpu.get_barrier_semaphore()

    @pl.loop(me + 1, dev)
    def _(d):
        pl.semaphore_signal(barrier, inc=1, device_id=coords(d), device_id_type=MESH)

    small = [
        pltpu.make_async_copy(src, dst, in_sem.at[n])
        for n, (src, dst) in enumerate((
            (lmo_hbm, lmo_ref), (ao_dom_hbm, ao_dom), (ao_cnt_hbm, ao_cnt),
            (pao_dom_hbm, pao_dom), (pao_cnt_hbm, pao_cnt), (order_hbm, order),
        ))
    ]
    for copy in small:
        copy.start()

    def load(p):
        return pltpu.make_async_copy(aux_hbm.at[p], aux.at[p], aux_sem.at[p])

    for p in range(rows):
        load(p).start()

    def coef_copy(slot, d):
        return pltpu.make_async_remote_copy(
            src_ref=lmo_ref, dst_ref=coef_all.at[slot],
            send_sem=coef_send.at[d], recv_sem=coef_recv.at[slot],
            device_id=coords(d), device_id_type=MESH,
        )

    @pl.when(me > 0)
    def _():
        pl.semaphore_wait(barrier, me)

    @pl.loop(0, me)
    def _(d):
        pl.semaphore_signal(entered.at[me], inc=1, device_id=coords(d), device_id_type=MESH)

    small[0].wait()

    @pl.loop(0, me)
    def _(d):
        coef_copy(me, d).start()

    coef_all[me] = lmo_ref[...]
    for copy in small[1:]:
        copy.wait()

    def greet(first, last):
        @pl.loop(first, last)
        def _(d):
            pl.semaphore_wait(entered.at[d], 1)
            coef_copy(me, d).start()

    eye = lax.broadcasted_iota(jnp.int32, (lmos, lmos), 0) == lax.broadcasted_iota(
        jnp.int32, (lmos, lmos), 1
    )
    where_to = []
    for k in range(DB):
        block = jnp.where(ao_cnt[...] > k, ao_dom[k:k + 1, :], -1).astype(jnp.float32)
        column = jnp.sum(jnp.where(eye, block, 0.0), axis=1, keepdims=True)
        where_to.append(jnp.broadcast_to(column, (lmos, BLK)))

    first = me + 1
    for p in range(max(rows, planes)):
        if p < planes:
            last = jnp.minimum(first + plane, dev)
            greet(first, last)
            first = last
        if p < rows:
            load(p).wait()
            aux_t[p] = aux[p].T

    @pl.loop(0, me)
    def _(d):
        coef_copy(d, d).wait_recv()

    @pl.loop(me + 1, dev)
    def _(d):
        coef_copy(d, d).wait_recv()

    for d in range(dev):
        coef32[d * per:(d + 1) * per, :] = coef_all[d].astype(jnp.float32)
    for b in range(blocks):
        total = jnp.zeros((lmos, BLK), jnp.float32)
        for k in range(DB):
            total = jnp.where(where_to[k] == b, coef32[:, k * BLK:(k + 1) * BLK], total)
        dense[:, b * BLK:(b + 1) * BLK] = total.astype(jnp.bfloat16)

    flat = half.reshape(lmos * blocks * rows, BLK)
    wide = 2
    for p in range(rows):
        for b in range(0, blocks, wide):
            out = jnp.dot(
                dense[...], aux_t[p, :, b * BLK:(b + wide) * BLK],
                preferred_element_type=jnp.float32,
            )
            for c in range(wide):
                flat[pl.ds((b + c) * rows + p, lmos, stride=blocks * rows), :] = (
                    out[:, c * BLK:(c + 1) * BLK]
                )

    def pack(d, dst):
        lmo = [order[d * per + j] for j in range(per)]
        cnt = [pao_cnt[i] for i in lmo]
        for s in range(USED):
            i, k = lmo[0], jnp.int32(s)
            start = jnp.int32(0)
            for j in range(1, per):
                start = start + cnt[j - 1]
                past = s >= start
                i = jnp.where(past, lmo[j], i)
                k = jnp.where(past, s - start, k)
            row = i * blocks + pao_dom[jnp.minimum(k, PB - 1), i]
            dst[s] = half[row].astype(jnp.bfloat16)

    def out_copy(slot, d):
        return pltpu.make_async_remote_copy(
            src_ref=send.at[d], dst_ref=recv.at[slot],
            send_sem=out_send.at[d], recv_sem=out_recv.at[slot],
            device_id=coords(d), device_id_type=MESH,
        )

    def target(t):
        i, j = t // plane, lax.rem(t, plane)
        own = i == planes - 1
        other = jnp.where(i >= my_plane, i + 1, i)
        return jnp.where(
            own,
            my_plane * plane + lax.rem(seat + 1 + j, plane),
            other * plane + lax.rem(seat + j, plane),
        )

    pack(target(0), send.at[target(0)])

    @pl.loop(0, dev - 2)
    def _(t):
        pack(target(t + 1), send.at[target(t + 1)])
        out_copy(me, target(t)).start()

    pack(me, recv.at[me])
    out_copy(me, target(dev - 2)).start()

    @pl.loop(0, dev - 1)
    def _(t):
        d = target(t)
        coef_copy(d, d).wait_send()
        out_copy(d, d).wait_send()

    @pl.loop(0, dev - 1)
    def _(t):
        d = target(t)
        out_copy(d, d).wait_recv()


def contract(n_lmo, per, recv, coef, pao_cnt, order, pair, metric, pair_out, metric_out, sem):
    me = lax.axis_index("aux") * n_lmo + lax.axis_index("lmo")
    dev, _, rows, _ = recv.shape
    start = jnp.int32(0)
    copies = []
    for g in range(per):
        count = pao_cnt[order[me * per + g]]
        tiles = []
        for k in range(PB):
            slot = jnp.minimum(start + k, USED - 1)
            tile = recv[:, slot].astype(jnp.float32).reshape(dev * rows, BLK)
            tiles.append(jnp.where(k < count, tile, 0.0).astype(jnp.bfloat16))
        start = start + count
        row = jnp.dot(
            jnp.concatenate(tiles, axis=1), coef[g], preferred_element_type=jnp.float32
        ).astype(jnp.bfloat16)
        pair_out[g] = row
        metric_out[g] = lax.dot_general(
            row, row, (((0,), (0,)), ((), ())), preferred_element_type=jnp.float32
        ) / (dev * rows)
        for c, (src, dst) in enumerate(((pair_out, pair), (metric_out, metric))):
            copies.append(pltpu.make_async_copy(src.at[g], dst.at[g], sem.at[g, c]))
            copies[-1].start()
    for copy in copies:
        copy.wait()


def shards(mesh, aux_ints, lmo_coef, ao_domain, ao_count, pao_domain, pao_count, owner_order, pao_coef):
    n_aux, n_lmo = mesh.shape["aux"], mesh.shape["lmo"]
    dev = n_aux * n_lmo
    rows, ao, _ = aux_ints.shape
    blocks = ao // BLK
    per = lmo_coef.shape[0]
    lmos = per * dev
    npao = pao_coef.shape[2]
    across = n_lmo // 2 if n_lmo % 2 == 0 and n_aux % (n_lmo // 2) == 0 else 1
    plane = across * n_lmo
    vmem = pl.BlockSpec(memory_space=pltpu.VMEM)
    smem = pl.BlockSpec(memory_space=pltpu.SMEM)
    anywhere = pl.BlockSpec(memory_space=pl.ANY)
    recv = pl.pallas_call(
        functools.partial(exchange, n_aux, n_lmo, plane),
        out_shape=pltpu.VMEM((dev, USED, rows, BLK), jnp.bfloat16),
        in_specs=[anywhere] * 7,
        out_specs=vmem,
        scratch_shapes=[
            pltpu.VMEM((rows, ao, ao), jnp.bfloat16),
            pltpu.VMEM((rows, ao, ao), jnp.bfloat16),
            pltpu.VMEM((per, DB * BLK), jnp.bfloat16),
            pltpu.VMEM((DB, lmos), jnp.int32),
            pltpu.VMEM((1, lmos), jnp.int32),
            pltpu.SMEM((PB, lmos), jnp.int32),
            pltpu.SMEM((lmos,), jnp.int32),
            pltpu.SMEM((lmos,), jnp.int32),
            pltpu.VMEM((dev, per, DB * BLK), jnp.bfloat16),
            pltpu.VMEM((lmos, DB * BLK), jnp.float32),
            pltpu.VMEM((lmos, ao), jnp.bfloat16),
            pltpu.VMEM((lmos * blocks, rows, BLK), jnp.float32),
            pltpu.VMEM((dev, USED, rows, BLK), jnp.bfloat16),
            pltpu.SemaphoreType.DMA((rows,)),
            pltpu.SemaphoreType.DMA((6,)),
            pltpu.SemaphoreType.REGULAR((dev,)),
            pltpu.SemaphoreType.DMA((dev,)),
            pltpu.SemaphoreType.DMA((dev,)),
            pltpu.SemaphoreType.DMA((dev,)),
            pltpu.SemaphoreType.DMA((dev,)),
        ],
        compiler_params=pltpu.CompilerParams(
            collective_id=0, has_side_effects=True, vmem_limit_bytes=48 * 2**20
        ),
        name="exchange",
    )(*(
        pltpu.with_memory_space_constraint(x, pltpu.HBM)
        for x in (aux_ints, lmo_coef, ao_domain.T, ao_count.reshape(1, lmos), pao_domain.T, pao_count, owner_order)
    ))
    pair, metric = pl.pallas_call(
        functools.partial(contract, n_lmo, per),
        out_shape=(
            jax.ShapeDtypeStruct((per, dev * rows, npao), jnp.bfloat16),
            jax.ShapeDtypeStruct((per, npao, npao), jnp.float32),
        ),
        in_specs=[vmem, vmem, smem, smem],
        out_specs=(anywhere, anywhere),
        scratch_shapes=[
            pltpu.VMEM((per, dev * rows, npao), jnp.bfloat16),
            pltpu.VMEM((per, npao, npao), jnp.float32),
            pltpu.SemaphoreType.DMA((per, 2)),
        ],
        compiler_params=pltpu.CompilerParams(vmem_limit_bytes=24 * 2**20),
        name="contract",
    )(recv, pao_coef, pao_count, owner_order)
    return pair, metric


def solution(mesh):
    split = ("aux", "lmo")
    placed = (P(split, None, None), P(split, None), P(), P(), P(), P(), P(), P(split, None, None))
    return jax.shard_map(
        functools.partial(shards, mesh),
        mesh=mesh,
        in_specs=placed,
        out_specs=(P(split, None, None), P(split, None, None)),
        check_vma=False,
    )
```

```python
import functools

import jax
import jax.numpy as jnp
from jax import lax
from jax.experimental import pallas as pl
from jax.experimental.pallas import tpu as pltpu
from jax.sharding import PartitionSpec as P

BLK = 128
DB = 3
PB = 3
USED = 8
MESH = pl.DeviceIdType.MESH


def exchange(
    n_aux, n_lmo, plane,
    aux_hbm, lmo_hbm, ao_dom_hbm, ao_cnt_hbm, pao_dom_hbm, pao_cnt_hbm, order_hbm, pao_hbm, pair,
    aux, aux_t, lmo_ref, ao_dom, ao_cnt, pao_dom, pao_cnt, order,
    coef_all, coef32, dense, half, send, recv, pao, pao_slots,
    aux_sem, in_sem, pao_sem, entered, coef_send, coef_recv, out_send, out_recv,
):
    dev = n_aux * n_lmo
    rows, ao, _ = aux_hbm.shape
    blocks = ao // BLK
    per = lmo_hbm.shape[0]
    lmos = per * dev
    planes = dev // plane
    pitch = half.shape[0] // lmos
    me = lax.axis_index("aux") * n_lmo + lax.axis_index("lmo")
    my_plane, seat = me // plane, lax.rem(me, plane)

    def coords(d):
        return (d // n_lmo, lax.rem(d, n_lmo))

    barrier = pltpu.get_barrier_semaphore()

    @pl.loop(me + 1, dev)
    def _(d):
        pl.semaphore_signal(barrier, inc=1, device_id=coords(d), device_id_type=MESH)

    small = [
        pltpu.make_async_copy(src, dst, in_sem.at[n])
        for n, (src, dst) in enumerate((
            (lmo_hbm, lmo_ref), (ao_dom_hbm, ao_dom), (ao_cnt_hbm, ao_cnt),
            (pao_dom_hbm, pao_dom), (pao_cnt_hbm, pao_cnt), (order_hbm, order),
        ))
    ]
    for copy in small:
        copy.start()

    def load(p):
        return pltpu.make_async_copy(aux_hbm.at[p], aux.at[p], aux_sem.at[p])

    for p in range(rows):
        load(p).start()
    pao_load = pltpu.make_async_copy(pao_hbm, pao, pao_sem)
    pao_load.start()

    def coef_copy(slot, d):
        return pltpu.make_async_remote_copy(
            src_ref=lmo_ref, dst_ref=coef_all.at[slot],
            send_sem=coef_send.at[d], recv_sem=coef_recv.at[slot],
            device_id=coords(d), device_id_type=MESH,
        )

    @pl.when(me > 0)
    def _():
        pl.semaphore_wait(barrier, me)

    @pl.loop(0, me)
    def _(d):
        pl.semaphore_signal(entered.at[me], inc=1, device_id=coords(d), device_id_type=MESH)

    small[0].wait()

    @pl.loop(0, me)
    def _(d):
        coef_copy(me, d).start()

    coef_all[me] = lmo_ref[...]
    for copy in small[1:]:
        copy.wait()

    def greet(first, last):
        @pl.loop(first, last)
        def _(d):
            pl.semaphore_wait(entered.at[d], 1)
            coef_copy(me, d).start()

    eye = lax.broadcasted_iota(jnp.int32, (lmos, lmos), 0) == lax.broadcasted_iota(
        jnp.int32, (lmos, lmos), 1
    )
    where_to = []
    for k in range(DB):
        block = jnp.where(ao_cnt[...] > k, ao_dom[k:k + 1, :], -1).astype(jnp.float32)
        column = jnp.sum(jnp.where(eye, block, 0.0), axis=1, keepdims=True)
        where_to.append(jnp.broadcast_to(column, (lmos, BLK)))

    first = me + 1
    for p in range(max(rows, planes)):
        if p < planes:
            last = jnp.minimum(first + plane, dev)
            greet(first, last)
            first = last
        if p < rows:
            load(p).wait()
            aux_t[p] = aux[p].T

    @pl.loop(0, me)
    def _(d):
        coef_copy(d, d).wait_recv()

    @pl.loop(me + 1, dev)
    def _(d):
        coef_copy(d, d).wait_recv()

    for d in range(dev):
        coef32[d * per:(d + 1) * per, :] = coef_all[d].astype(jnp.float32)
    for b in range(blocks):
        total = jnp.zeros((lmos, BLK), jnp.float32)
        for k in range(DB):
            total = jnp.where(where_to[k] == b, coef32[:, k * BLK:(k + 1) * BLK], total)
        dense[:, b * BLK:(b + 1) * BLK] = total.astype(jnp.bfloat16)

    wide = 2
    for p in range(rows):
        for b in range(0, blocks, wide):
            out = jnp.dot(
                dense[...], aux_t[p, :, b * BLK:(b + wide) * BLK],
                preferred_element_type=jnp.float32,
            )
            for c in range(wide):
                half[pl.ds((b + c) * rows + p, lmos, stride=pitch), :] = (
                    out[:, c * BLK:(c + 1) * BLK]
                )

    def pack(d, dst):
        lmo = [order[d * per + j] for j in range(per)]
        cnt = [pao_cnt[i] for i in lmo]
        for s in range(USED):
            i, k = lmo[0], jnp.int32(s)
            start = jnp.int32(0)
            for j in range(1, per):
                start = start + cnt[j - 1]
                past = s >= start
                i = jnp.where(past, lmo[j], i)
                k = jnp.where(past, s - start, k)
            row = i * pitch + pao_dom[jnp.minimum(k, PB - 1), i] * rows
            dst[s] = half[pl.ds(row, rows), :].astype(jnp.bfloat16)

    def out_copy(slot, d):
        return pltpu.make_async_remote_copy(
            src_ref=send.at[d], dst_ref=recv.at[slot],
            send_sem=out_send.at[d], recv_sem=out_recv.at[slot],
            device_id=coords(d), device_id_type=MESH,
        )

    def target(t):
        i, j = t // plane, lax.rem(t, plane)
        own = i == planes - 1
        other = jnp.where(i >= my_plane, i + 1, i)
        return jnp.where(
            own,
            my_plane * plane + lax.rem(seat + 1 + j, plane),
            other * plane + lax.rem(seat + j, plane),
        )

    pack(target(0), send.at[target(0)])

    @pl.loop(0, dev - 2)
    def _(t):
        pack(target(t + 1), send.at[target(t + 1)])
        out_copy(me, target(t)).start()

    pack(me, recv.at[me])
    out_copy(me, target(dev - 2)).start()

    @pl.loop(0, dev - 1)
    def _(t):
        d = target(t)
        coef_copy(d, d).wait_send()
        out_copy(d, d).wait_send()

    npao = pao.shape[3]
    pao_load.wait()
    start = jnp.int32(0)
    for g in range(per):
        count = pao_cnt[order[me * per + g]]
        for s in range(USED):
            k = s - start
            tile = pao[g, jnp.clip(k, 0, PB - 1)]
            pao_slots[s * BLK:(s + 1) * BLK, g * npao:(g + 1) * npao] = jnp.where(
                (k >= 0) & (k < count), tile, jnp.zeros_like(tile)
            )
        start = start + count

    def project(i):
        @pl.loop(0, plane)
        def _(j):
            d = i * plane + j

            @pl.when(d != me)
            def _():
                out_copy(d, d).wait_recv()

        first = pl.multiple_of(i * plane, plane)
        here = jnp.concatenate([
            recv[pl.ds(first, plane), s].astype(jnp.float32).reshape(plane * rows, BLK).astype(jnp.bfloat16)
            for s in range(USED)
        ], axis=1)
        to = pl.multiple_of(i * (plane * rows), plane * rows)
        for g in range(per):
            pair[g, pl.ds(to, plane * rows), :] = jnp.dot(
                here, pao_slots[:, g * npao:(g + 1) * npao], preferred_element_type=jnp.float32
            ).astype(jnp.bfloat16)

    project(jnp.where(my_plane == 0, 1, 0) if planes > 1 else my_plane)
    if planes > 1:
        project(my_plane)
    for i in range(1, planes - 1):
        project(jnp.where(i >= my_plane, i + 1, i))


def contract(pair, pair_out, metric_out, metric, pair_sem, metric_sem):
    per, total, _ = pair.shape
    copies = [pltpu.make_async_copy(pair, pair_out, pair_sem)]
    copies[0].start()
    for g in range(per):
        row = pair[g]
        metric[g] = lax.dot_general(
            row, row, (((0,), (0,)), ((), ())), preferred_element_type=jnp.float32
        ) / total
        copies.append(pltpu.make_async_copy(metric.at[g], metric_out.at[g], metric_sem.at[g]))
        copies[-1].start()
    for copy in copies:
        copy.wait()


def shards(mesh, aux_ints, lmo_coef, ao_domain, ao_count, pao_domain, pao_count, owner_order, pao_coef):
    n_aux, n_lmo = mesh.shape["aux"], mesh.shape["lmo"]
    dev = n_aux * n_lmo
    rows, ao, _ = aux_ints.shape
    blocks = ao // BLK
    per = lmo_coef.shape[0]
    lmos = per * dev
    npao = pao_coef.shape[2]
    across = n_lmo // 2 if n_lmo % 2 == 0 and n_aux % (n_lmo // 2) == 0 else 1
    plane = across * n_lmo
    vmem = pl.BlockSpec(memory_space=pltpu.VMEM)
    anywhere = pl.BlockSpec(memory_space=pl.ANY)
    pair = pl.pallas_call(
        functools.partial(exchange, n_aux, n_lmo, plane),
        out_shape=pltpu.VMEM((per, dev * rows, npao), jnp.bfloat16),
        in_specs=[anywhere] * 8,
        out_specs=vmem,
        scratch_shapes=[
            pltpu.VMEM((rows, ao, ao), jnp.bfloat16),
            pltpu.VMEM((rows, ao, ao), jnp.bfloat16),
            pltpu.VMEM((per, DB * BLK), jnp.bfloat16),
            pltpu.VMEM((DB, lmos), jnp.int32),
            pltpu.VMEM((1, lmos), jnp.int32),
            pltpu.SMEM((PB, lmos), jnp.int32),
            pltpu.SMEM((lmos,), jnp.int32),
            pltpu.SMEM((lmos,), jnp.int32),
            pltpu.VMEM((dev, per, DB * BLK), jnp.bfloat16),
            pltpu.VMEM((lmos, DB * BLK), jnp.float32),
            pltpu.VMEM((lmos, ao), jnp.bfloat16),
            pltpu.VMEM((lmos * (blocks * rows + 4), BLK), jnp.float32),
            pltpu.VMEM((dev, USED, rows, BLK), jnp.bfloat16),
            pltpu.VMEM((dev, USED, rows, BLK), jnp.bfloat16),
            pltpu.VMEM((per, PB, BLK, npao), jnp.bfloat16),
            pltpu.VMEM((USED * BLK, per * npao), jnp.bfloat16),
            pltpu.SemaphoreType.DMA((rows,)),
            pltpu.SemaphoreType.DMA((6,)),
            pltpu.SemaphoreType.DMA,
            pltpu.SemaphoreType.REGULAR((dev,)),
            pltpu.SemaphoreType.DMA((dev,)),
            pltpu.SemaphoreType.DMA((dev,)),
            pltpu.SemaphoreType.DMA((dev,)),
            pltpu.SemaphoreType.DMA((dev,)),
        ],
        compiler_params=pltpu.CompilerParams(
            collective_id=0, has_side_effects=True, vmem_limit_bytes=48 * 2**20
        ),
        name="exchange",
    )(*(
        pltpu.with_memory_space_constraint(x, pltpu.HBM)
        for x in (
            aux_ints, lmo_coef, ao_domain.T, ao_count.reshape(1, lmos), pao_domain.T, pao_count,
            owner_order, pao_coef.reshape(per, PB, BLK, npao),
        )
    ))
    return pl.pallas_call(
        contract,
        out_shape=(
            jax.ShapeDtypeStruct((per, dev * rows, npao), jnp.bfloat16),
            jax.ShapeDtypeStruct((per, npao, npao), jnp.float32),
        ),
        in_specs=[vmem],
        out_specs=(anywhere, anywhere),
        scratch_shapes=[
            pltpu.VMEM((per, npao, npao), jnp.float32),
            pltpu.SemaphoreType.DMA,
            pltpu.SemaphoreType.DMA((per,)),
        ],
        compiler_params=pltpu.CompilerParams(vmem_limit_bytes=16 * 2**20),
        name="contract",
    )(pair)


def solution(mesh):
    split = ("aux", "lmo")
    placed = (P(split, None, None), P(split, None), P(), P(), P(), P(), P(), P(split, None, None))
    return jax.shard_map(
        functools.partial(shards, mesh),
        mesh=mesh,
        in_specs=placed,
        out_specs=(P(split, None, None), P(split, None, None)),
        check_vma=False,
    )
```

```python
import functools

import jax
import jax.numpy as jnp
from jax import lax
from jax.experimental import pallas as pl
from jax.experimental.pallas import tpu as pltpu
from jax.sharding import PartitionSpec as P

BLK = 128
DB = 3
PB = 3
USED = 8
MESH = pl.DeviceIdType.MESH


def exchange(
    n_aux, n_lmo, plane,
    aux_hbm, lmo_hbm, ao_dom_hbm, ao_cnt_hbm, pao_dom_hbm, pao_cnt_hbm, order_hbm, pao_hbm, pair,
    aux, aux_t, lmo_ref, ao_dom, ao_cnt, pao_dom, pao_cnt, order,
    coef_all, coef32, dense, half, send, recv, pao, pao_slots,
    aux_sem, in_sem, pao_sem, entered, coef_send, coef_recv, out_send, out_recv,
):
    dev = n_aux * n_lmo
    rows, ao, _ = aux_hbm.shape
    blocks = ao // BLK
    per = lmo_hbm.shape[0]
    lmos = per * dev
    planes = dev // plane
    pitch = half.shape[0] // lmos
    me = lax.axis_index("aux") * n_lmo + lax.axis_index("lmo")
    my_plane, seat = me // plane, lax.rem(me, plane)

    def coords(d):
        return (d // n_lmo, lax.rem(d, n_lmo))

    barrier = pltpu.get_barrier_semaphore()

    @pl.loop(me + 1, dev)
    def _(d):
        pl.semaphore_signal(barrier, inc=1, device_id=coords(d), device_id_type=MESH)

    small = [
        pltpu.make_async_copy(src, dst, in_sem.at[n])
        for n, (src, dst) in enumerate((
            (lmo_hbm, lmo_ref), (ao_dom_hbm, ao_dom), (ao_cnt_hbm, ao_cnt),
            (pao_dom_hbm, pao_dom), (pao_cnt_hbm, pao_cnt), (order_hbm, order),
        ))
    ]
    for copy in small:
        copy.start()

    def load(p):
        return pltpu.make_async_copy(aux_hbm.at[p], aux.at[p], aux_sem.at[p])

    for p in range(rows):
        load(p).start()
    pao_load = pltpu.make_async_copy(pao_hbm, pao, pao_sem)
    pao_load.start()

    def coef_copy(slot, d):
        return pltpu.make_async_remote_copy(
            src_ref=lmo_ref, dst_ref=coef_all.at[slot],
            send_sem=coef_send.at[d], recv_sem=coef_recv.at[slot],
            device_id=coords(d), device_id_type=MESH,
        )

    @pl.when(me > 0)
    def _():
        pl.semaphore_wait(barrier, me)

    @pl.loop(0, me)
    def _(d):
        pl.semaphore_signal(entered.at[me], inc=1, device_id=coords(d), device_id_type=MESH)

    small[0].wait()

    @pl.loop(0, me)
    def _(d):
        coef_copy(me, d).start()

    coef_all[me] = lmo_ref[...]
    for copy in small[1:]:
        copy.wait()

    def greet(first, last):
        @pl.loop(first, last)
        def _(d):
            pl.semaphore_wait(entered.at[d], 1)
            coef_copy(me, d).start()

    eye = lax.broadcasted_iota(jnp.int32, (lmos, lmos), 0) == lax.broadcasted_iota(
        jnp.int32, (lmos, lmos), 1
    )
    where_to = []
    for k in range(DB):
        block = jnp.where(ao_cnt[...] > k, ao_dom[k:k + 1, :], -1).astype(jnp.float32)
        column = jnp.sum(jnp.where(eye, block, 0.0), axis=1, keepdims=True)
        where_to.append(jnp.broadcast_to(column, (lmos, BLK)))

    first = me + 1
    for p in range(max(rows, planes)):
        if p < planes:
            last = jnp.minimum(first + plane, dev)
            greet(first, last)
            first = last
        if p < rows:
            load(p).wait()
            aux_t[p] = aux[p].T

    @pl.loop(0, me)
    def _(d):
        coef_copy(d, d).wait_recv()

    @pl.loop(me + 1, dev)
    def _(d):
        coef_copy(d, d).wait_recv()

    for d in range(dev):
        coef32[d * per:(d + 1) * per, :] = coef_all[d].astype(jnp.float32)
    for b in range(blocks):
        total = jnp.zeros((lmos, BLK), jnp.float32)
        for k in range(DB):
            total = jnp.where(where_to[k] == b, coef32[:, k * BLK:(k + 1) * BLK], total)
        dense[:, b * BLK:(b + 1) * BLK] = total.astype(jnp.bfloat16)

    wide = 2
    for p in range(rows):
        for b in range(0, blocks, wide):
            out = jnp.dot(
                dense[...], aux_t[p, :, b * BLK:(b + wide) * BLK],
                preferred_element_type=jnp.float32,
            )
            for c in range(wide):
                half[pl.ds((b + c) * rows + p, lmos, stride=pitch), :] = (
                    out[:, c * BLK:(c + 1) * BLK]
                )

    def pack(d, dst):
        lmo = [order[d * per + j] for j in range(per)]
        cnt = [pao_cnt[i] for i in lmo]
        for s in range(USED):
            i, k = lmo[0], jnp.int32(s)
            start = jnp.int32(0)
            for j in range(1, per):
                start = start + cnt[j - 1]
                past = s >= start
                i = jnp.where(past, lmo[j], i)
                k = jnp.where(past, s - start, k)
            row = i * pitch + pao_dom[jnp.minimum(k, PB - 1), i] * rows
            dst[s] = half[pl.ds(row, rows), :].astype(jnp.bfloat16)

    def out_copy(slot, d):
        return pltpu.make_async_remote_copy(
            src_ref=send.at[d], dst_ref=recv.at[slot],
            send_sem=out_send.at[d], recv_sem=out_recv.at[slot],
            device_id=coords(d), device_id_type=MESH,
        )

    def target(t):
        i, j = t // plane, lax.rem(t, plane)
        own = i == planes - 1
        other = jnp.where(i >= my_plane, i + 1, i)
        return jnp.where(
            own,
            my_plane * plane + lax.rem(seat + 1 + j, plane),
            other * plane + lax.rem(seat + j, plane),
        )

    pack(target(0), send.at[target(0)])

    @pl.loop(0, dev - 2)
    def _(t):
        pack(target(t + 1), send.at[target(t + 1)])
        out_copy(me, target(t)).start()

    pack(me, recv.at[me])
    out_copy(me, target(dev - 2)).start()

    npao = pao.shape[3]
    pao_load.wait()
    start = jnp.int32(0)
    for g in range(per):
        count = pao_cnt[order[me * per + g]]
        for s in range(USED):
            k = s - start
            tile = pao[g, jnp.clip(k, 0, PB - 1)]
            pao_slots[s * BLK:(s + 1) * BLK, g * npao:(g + 1) * npao] = jnp.where(
                (k >= 0) & (k < count), tile, jnp.zeros_like(tile)
            )
        start = start + count

    def project(i):
        @pl.loop(0, plane)
        def _(j):
            d = i * plane + j

            @pl.when(d != me)
            def _():
                out_copy(d, d).wait_recv()

        first = pl.multiple_of(i * plane, plane)
        here = jnp.concatenate([
            recv[pl.ds(first, plane), s].astype(jnp.float32).reshape(plane * rows, BLK).astype(jnp.bfloat16)
            for s in range(USED)
        ], axis=1)
        to = pl.multiple_of(i * (plane * rows), plane * rows)
        for g in range(per):
            pair[g, pl.ds(to, plane * rows), :] = jnp.dot(
                here, pao_slots[:, g * npao:(g + 1) * npao], preferred_element_type=jnp.float32
            ).astype(jnp.bfloat16)

    def drain():
        @pl.loop(0, dev - 1)
        def _(t):
            d = target(t)
            coef_copy(d, d).wait_send()
            out_copy(d, d).wait_send()

    arrivals = [jnp.where(my_plane == 0, 1, 0), my_plane] if planes > 1 else [my_plane]
    arrivals += [jnp.where(i >= my_plane, i + 1, i) for i in range(1, planes - 1)]
    for n, i in enumerate(arrivals):
        if n == planes - 1:
            drain()
        project(i)


def contract(pair, pair_out, metric_out, metric, pair_sem, metric_sem):
    per, total, _ = pair.shape
    copies = [pltpu.make_async_copy(pair, pair_out, pair_sem)]
    copies[0].start()
    for g in range(per):
        row = pair[g]
        metric[g] = lax.dot_general(
            row, row, (((0,), (0,)), ((), ())), preferred_element_type=jnp.float32
        ) / total
        copies.append(pltpu.make_async_copy(metric.at[g], metric_out.at[g], metric_sem.at[g]))
        copies[-1].start()
    for copy in copies:
        copy.wait()


def shards(mesh, aux_ints, lmo_coef, ao_domain, ao_count, pao_domain, pao_count, owner_order, pao_coef):
    n_aux, n_lmo = mesh.shape["aux"], mesh.shape["lmo"]
    dev = n_aux * n_lmo
    rows, ao, _ = aux_ints.shape
    blocks = ao // BLK
    per = lmo_coef.shape[0]
    lmos = per * dev
    npao = pao_coef.shape[2]
    across = n_lmo // 2 if n_lmo % 2 == 0 and n_aux % (n_lmo // 2) == 0 else 1
    plane = across * n_lmo
    vmem = pl.BlockSpec(memory_space=pltpu.VMEM)
    anywhere = pl.BlockSpec(memory_space=pl.ANY)
    pair = pl.pallas_call(
        functools.partial(exchange, n_aux, n_lmo, plane),
        out_shape=pltpu.VMEM((per, dev * rows, npao), jnp.bfloat16),
        in_specs=[anywhere] * 8,
        out_specs=vmem,
        scratch_shapes=[
            pltpu.VMEM((rows, ao, ao), jnp.bfloat16),
            pltpu.VMEM((rows, ao, ao), jnp.bfloat16),
            pltpu.VMEM((per, DB * BLK), jnp.bfloat16),
            pltpu.VMEM((DB, lmos), jnp.int32),
            pltpu.VMEM((1, lmos), jnp.int32),
            pltpu.SMEM((PB, lmos), jnp.int32),
            pltpu.SMEM((lmos,), jnp.int32),
            pltpu.SMEM((lmos,), jnp.int32),
            pltpu.VMEM((dev, per, DB * BLK), jnp.bfloat16),
            pltpu.VMEM((lmos, DB * BLK), jnp.float32),
            pltpu.VMEM((lmos, ao), jnp.bfloat16),
            pltpu.VMEM((lmos * (blocks * rows + 4), BLK), jnp.float32),
            pltpu.VMEM((dev, USED, rows, BLK), jnp.bfloat16),
            pltpu.VMEM((dev, USED, rows, BLK), jnp.bfloat16),
            pltpu.VMEM((per, PB, BLK, npao), jnp.bfloat16),
            pltpu.VMEM((USED * BLK, per * npao), jnp.bfloat16),
            pltpu.SemaphoreType.DMA((rows,)),
            pltpu.SemaphoreType.DMA((6,)),
            pltpu.SemaphoreType.DMA,
            pltpu.SemaphoreType.REGULAR((dev,)),
            pltpu.SemaphoreType.DMA((dev,)),
            pltpu.SemaphoreType.DMA((dev,)),
            pltpu.SemaphoreType.DMA((dev,)),
            pltpu.SemaphoreType.DMA((dev,)),
        ],
        compiler_params=pltpu.CompilerParams(
            collective_id=0, has_side_effects=True, vmem_limit_bytes=48 * 2**20
        ),
        name="exchange",
    )(*(
        pltpu.with_memory_space_constraint(x, pltpu.HBM)
        for x in (
            aux_ints, lmo_coef, ao_domain.T, ao_count.reshape(1, lmos), pao_domain.T, pao_count,
            owner_order, pao_coef.reshape(per, PB, BLK, npao),
        )
    ))
    return pl.pallas_call(
        contract,
        out_shape=(
            jax.ShapeDtypeStruct((per, dev * rows, npao), jnp.bfloat16),
            jax.ShapeDtypeStruct((per, npao, npao), jnp.float32),
        ),
        in_specs=[vmem],
        out_specs=(anywhere, anywhere),
        scratch_shapes=[
            pltpu.VMEM((per, npao, npao), jnp.float32),
            pltpu.SemaphoreType.DMA,
            pltpu.SemaphoreType.DMA((per,)),
        ],
        compiler_params=pltpu.CompilerParams(vmem_limit_bytes=16 * 2**20),
        name="contract",
    )(pair)


def solution(mesh):
    split = ("aux", "lmo")
    placed = (P(split, None, None), P(split, None), P(), P(), P(), P(), P(), P(split, None, None))
    return jax.shard_map(
        functools.partial(shards, mesh),
        mesh=mesh,
        in_specs=placed,
        out_specs=(P(split, None, None), P(split, None, None)),
        check_vma=False,
    )
```

```python
import functools

import jax
import jax.numpy as jnp
from jax import lax
from jax.experimental import pallas as pl
from jax.experimental.pallas import tpu as pltpu
from jax.sharding import PartitionSpec as P

BLK = 128
DB = 3
PB = 3
USED = 8
MESH = pl.DeviceIdType.MESH


def exchange(
    n_aux, n_lmo, plane,
    aux_hbm, lmo_hbm, ao_dom_hbm, ao_cnt_hbm, pao_dom_hbm, pao_cnt_hbm, order_hbm, pao_hbm, pair,
    aux, aux_t, lmo_ref, ao_dom, ao_cnt, pao_dom, pao_cnt, order,
    coef_all, coef32, dense, half, send, recv, pao, pao_slots,
    aux_sem, in_sem, pao_sem, entered, coef_send, coef_recv, out_send, out_recv,
):
    dev = n_aux * n_lmo
    rows, ao, _ = aux_hbm.shape
    blocks = ao // BLK
    per = lmo_hbm.shape[0]
    lmos = per * dev
    planes = dev // plane
    pitch = half.shape[0] // lmos
    me = lax.axis_index("aux") * n_lmo + lax.axis_index("lmo")
    my_plane, seat = me // plane, lax.rem(me, plane)

    def coords(d):
        return (d // n_lmo, lax.rem(d, n_lmo))

    barrier = pltpu.get_barrier_semaphore()
    before = dev - plane
    in_last = my_plane == planes - 1

    def others(first, last, act):
        @pl.loop(first, last)
        def _(d):
            @pl.when(d != me)
            def _():
                act(d)

    others(
        jnp.where(in_last, before, 0), dev,
        lambda d: pl.semaphore_signal(barrier, inc=1, device_id=coords(d), device_id_type=MESH),
    )

    small = [
        pltpu.make_async_copy(src, dst, in_sem.at[n])
        for n, (src, dst) in enumerate((
            (lmo_hbm, lmo_ref), (ao_dom_hbm, ao_dom), (ao_cnt_hbm, ao_cnt),
            (pao_dom_hbm, pao_dom), (pao_cnt_hbm, pao_cnt), (order_hbm, order),
        ))
    ]
    for copy in small:
        copy.start()

    def load(p):
        return pltpu.make_async_copy(aux_hbm.at[p], aux.at[p], aux_sem.at[p])

    for p in range(rows):
        load(p).start()
    pao_load = pltpu.make_async_copy(pao_hbm, pao, pao_sem)
    pao_load.start()

    def coef_copy(slot, d):
        return pltpu.make_async_remote_copy(
            src_ref=lmo_ref, dst_ref=coef_all.at[slot],
            send_sem=coef_send, recv_sem=coef_recv,
            device_id=coords(d), device_id_type=MESH,
        )

    @pl.when(in_last)
    def _():
        pl.semaphore_wait(barrier, dev - 1)

        @pl.loop(0, before)
        def _(d):
            pl.semaphore_signal(entered.at[me], inc=1, device_id=coords(d), device_id_type=MESH)

    if planes > 1:
        @pl.when(jnp.logical_not(in_last))
        def _():
            pl.semaphore_wait(barrier, before - 1)

    small[0].wait()
    for i in range(planes - 2, -1, -1):
        others(i * plane, (i + 1) * plane, lambda d: coef_copy(me, d).start())
    others(before, jnp.where(in_last, dev, before), lambda d: coef_copy(me, d).start())

    coef_all[me] = lmo_ref[...]
    for copy in small[1:]:
        copy.wait()

    eye = lax.broadcasted_iota(jnp.int32, (lmos, lmos), 0) == lax.broadcasted_iota(
        jnp.int32, (lmos, lmos), 1
    )
    where_to = []
    for k in range(DB):
        block = jnp.where(ao_cnt[...] > k, ao_dom[k:k + 1, :], -1).astype(jnp.float32)
        column = jnp.sum(jnp.where(eye, block, 0.0), axis=1, keepdims=True)
        where_to.append(jnp.broadcast_to(column, (lmos, BLK)))

    def turn(p):
        load(p).wait()
        aux_t[p] = aux[p].T

    for p in range(rows // 2):
        turn(p)

    @pl.loop(before, jnp.where(in_last, before, dev))
    def _(d):
        pl.semaphore_wait(entered.at[d], 1)
        coef_copy(me, d).start()

    for p in range(rows // 2, rows):
        turn(p)

    all_coefs = pltpu.make_async_remote_copy(
        src_ref=coef_all.at[pl.ds(0, dev - 1)], dst_ref=coef_all.at[pl.ds(0, dev - 1)],
        send_sem=coef_send, recv_sem=coef_recv,
        device_id=coords(me), device_id_type=MESH,
    )
    all_coefs.wait_recv()

    for d in range(dev):
        coef32[d * per:(d + 1) * per, :] = coef_all[d].astype(jnp.float32)
    for b in range(blocks):
        total = jnp.zeros((lmos, BLK), jnp.float32)
        for k in range(DB):
            total = jnp.where(where_to[k] == b, coef32[:, k * BLK:(k + 1) * BLK], total)
        dense[:, b * BLK:(b + 1) * BLK] = total.astype(jnp.bfloat16)

    wide = 2
    for p in range(rows):
        for b in range(0, blocks, wide):
            out = jnp.dot(
                dense[...], aux_t[p, :, b * BLK:(b + wide) * BLK],
                preferred_element_type=jnp.float32,
            )
            for c in range(wide):
                half[pl.ds((b + c) * rows + p, lmos, stride=pitch), :] = (
                    out[:, c * BLK:(c + 1) * BLK]
                )

    def pack(d, dst):
        lmo = [order[d * per + j] for j in range(per)]
        cnt = [pao_cnt[i] for i in lmo]
        for s in range(USED):
            i, k = lmo[0], jnp.int32(s)
            start = jnp.int32(0)
            for j in range(1, per):
                start = start + cnt[j - 1]
                past = s >= start
                i = jnp.where(past, lmo[j], i)
                k = jnp.where(past, s - start, k)
            row = i * pitch + pao_dom[jnp.minimum(k, PB - 1), i] * rows
            dst[s] = half[pl.ds(row, rows), :].astype(jnp.bfloat16)

    def out_copy(slot, d):
        return pltpu.make_async_remote_copy(
            src_ref=send.at[d], dst_ref=recv.at[slot],
            send_sem=out_send, recv_sem=out_recv.at[slot // plane],
            device_id=coords(d), device_id_type=MESH,
        )

    def rows_of(first, count, sem):
        return pltpu.make_async_remote_copy(
            src_ref=send.at[pl.ds(first, count)], dst_ref=recv.at[pl.ds(first, count)],
            send_sem=out_send, recv_sem=sem,
            device_id=coords(me), device_id_type=MESH,
        )

    half_way = planes // 2

    def target(t):
        i, j = t // plane, lax.rem(t, plane)
        down = planes - 1 - i
        other = jnp.where(
            my_plane < half_way,
            jnp.where(down <= my_plane, down - 1, down),
            jnp.where(i >= my_plane, i + 1, i),
        )
        if planes > 2:
            other = jnp.where(in_last, jnp.where(i == 0, planes - 2, i - 1), other)
        return jnp.where(
            i >= planes - 1,
            my_plane * plane + lax.rem(seat + 1 + j, plane),
            other * plane + lax.rem(seat + j, plane),
        )

    pack(target(0), send.at[target(0)])

    @pl.loop(0, dev - 2)
    def _(t):
        pack(target(t + 1), send.at[target(t + 1)])
        out_copy(me, target(t)).start()

    pack(me, recv.at[me])
    out_copy(me, target(dev - 2)).start()

    npao = pao.shape[3]
    pao_load.wait()
    start = jnp.int32(0)
    for g in range(per):
        count = pao_cnt[order[me * per + g]]
        for s in range(USED):
            k = s - start
            tile = pao[g, jnp.clip(k, 0, PB - 1)]
            pao_slots[s * BLK:(s + 1) * BLK, g * npao:(g + 1) * npao] = jnp.where(
                (k >= 0) & (k < count), tile, jnp.zeros_like(tile)
            )
        start = start + count

    def project(n, i):
        first = pl.multiple_of(i * plane, plane)
        own = n == 0
        rows_of(first, plane - own, out_recv.at[i]).wait_recv()
        here = jnp.concatenate([
            recv[pl.ds(first, plane), s].astype(jnp.float32).reshape(plane * rows, BLK).astype(jnp.bfloat16)
            for s in range(USED)
        ], axis=1)
        to = pl.multiple_of(i * (plane * rows), plane * rows)
        for g in range(per):
            pair[g, pl.ds(to, plane * rows), :] = jnp.dot(
                here, pao_slots[:, g * npao:(g + 1) * npao], preferred_element_type=jnp.float32
            ).astype(jnp.bfloat16)

    last = jnp.where(my_plane < half_way, half_way, half_way - 1)
    low, high = jnp.minimum(my_plane, last), jnp.maximum(my_plane, last)
    arrivals = [my_plane]
    for n in range(planes - 2):
        i = planes - 1 - n
        i = jnp.where(i <= high, i - 1, i)
        arrivals.append(jnp.where(i <= low, i - 1, i))
    if planes > 1:
        arrivals.append(last)
    for n, i in enumerate(arrivals):
        project(n, i)
    all_coefs.wait_send()
    rows_of(0, dev - 1, out_recv.at[0]).wait_send()


def contract(pair, pair_out, metric_out, metric, pair_sem, metric_sem):
    per, total, _ = pair.shape
    copies = [pltpu.make_async_copy(pair, pair_out, pair_sem)]
    copies[0].start()
    for g in range(per):
        row = pair[g]
        metric[g] = lax.dot_general(
            row, row, (((0,), (0,)), ((), ())), preferred_element_type=jnp.float32
        ) / total
        copies.append(pltpu.make_async_copy(metric.at[g], metric_out.at[g], metric_sem.at[g]))
        copies[-1].start()
    for copy in copies:
        copy.wait()


def shards(mesh, aux_ints, lmo_coef, ao_domain, ao_count, pao_domain, pao_count, owner_order, pao_coef):
    n_aux, n_lmo = mesh.shape["aux"], mesh.shape["lmo"]
    dev = n_aux * n_lmo
    rows, ao, _ = aux_ints.shape
    blocks = ao // BLK
    per = lmo_coef.shape[0]
    lmos = per * dev
    npao = pao_coef.shape[2]
    across = n_lmo // 2 if n_lmo % 2 == 0 and n_aux % (n_lmo // 2) == 0 else 1
    plane = across * n_lmo
    vmem = pl.BlockSpec(memory_space=pltpu.VMEM)
    anywhere = pl.BlockSpec(memory_space=pl.ANY)
    pair = pl.pallas_call(
        functools.partial(exchange, n_aux, n_lmo, plane),
        out_shape=pltpu.VMEM((per, dev * rows, npao), jnp.bfloat16),
        in_specs=[anywhere] * 8,
        out_specs=vmem,
        scratch_shapes=[
            pltpu.VMEM((rows, ao, ao), jnp.bfloat16),
            pltpu.VMEM((rows, ao, ao), jnp.bfloat16),
            pltpu.VMEM((per, DB * BLK), jnp.bfloat16),
            pltpu.VMEM((DB, lmos), jnp.int32),
            pltpu.VMEM((1, lmos), jnp.int32),
            pltpu.SMEM((PB, lmos), jnp.int32),
            pltpu.SMEM((lmos,), jnp.int32),
            pltpu.SMEM((lmos,), jnp.int32),
            pltpu.VMEM((dev, per, DB * BLK), jnp.bfloat16),
            pltpu.VMEM((lmos, DB * BLK), jnp.float32),
            pltpu.VMEM((lmos, ao), jnp.bfloat16),
            pltpu.VMEM((lmos * (blocks * rows + 4), BLK), jnp.float32),
            pltpu.VMEM((dev, USED, rows, BLK), jnp.bfloat16),
            pltpu.VMEM((dev, USED, rows, BLK), jnp.bfloat16),
            pltpu.VMEM((per, PB, BLK, npao), jnp.bfloat16),
            pltpu.VMEM((USED * BLK, per * npao), jnp.bfloat16),
            pltpu.SemaphoreType.DMA((rows,)),
            pltpu.SemaphoreType.DMA((6,)),
            pltpu.SemaphoreType.DMA,
            pltpu.SemaphoreType.REGULAR((dev,)),
            pltpu.SemaphoreType.DMA,
            pltpu.SemaphoreType.DMA,
            pltpu.SemaphoreType.DMA,
            pltpu.SemaphoreType.DMA((dev // plane,)),
        ],
        compiler_params=pltpu.CompilerParams(
            collective_id=0, has_side_effects=True, vmem_limit_bytes=48 * 2**20
        ),
        name="exchange",
    )(*(
        pltpu.with_memory_space_constraint(x, pltpu.HBM)
        for x in (
            aux_ints, lmo_coef, ao_domain.T, ao_count.reshape(1, lmos), pao_domain.T, pao_count,
            owner_order, pao_coef.reshape(per, PB, BLK, npao),
        )
    ))
    return pl.pallas_call(
        contract,
        out_shape=(
            jax.ShapeDtypeStruct((per, dev * rows, npao), jnp.bfloat16),
            jax.ShapeDtypeStruct((per, npao, npao), jnp.float32),
        ),
        in_specs=[vmem],
        out_specs=(anywhere, anywhere),
        scratch_shapes=[
            pltpu.VMEM((per, npao, npao), jnp.float32),
            pltpu.SemaphoreType.DMA,
            pltpu.SemaphoreType.DMA((per,)),
        ],
        compiler_params=pltpu.CompilerParams(vmem_limit_bytes=16 * 2**20),
        name="contract",
    )(pair)


def solution(mesh):
    split = ("aux", "lmo")
    placed = (P(split, None, None), P(split, None), P(), P(), P(), P(), P(), P(split, None, None))
    return jax.shard_map(
        functools.partial(shards, mesh),
        mesh=mesh,
        in_specs=placed,
        out_specs=(P(split, None, None), P(split, None, None)),
        check_vma=False,
    )
```

```python
import functools

import jax
import jax.numpy as jnp
from jax import lax
from jax.experimental import pallas as pl
from jax.experimental.pallas import tpu as pltpu
from jax.sharding import PartitionSpec as P

BLK = 128
DB = 3
PB = 3
USED = 8
MESH = pl.DeviceIdType.MESH


def exchange(
    n_aux, n_lmo, plane,
    aux_hbm, lmo_hbm, ao_dom_hbm, ao_cnt_hbm, pao_dom_hbm, pao_cnt_hbm, order_hbm, pao_hbm, pair,
    aux, aux_t, lmo_ref, ao_dom, ao_cnt, pao_dom, pao_cnt, order,
    coef_all, coef32, dense, half, send, recv, pao, pao_slots,
    aux_sem, in_sem, pao_sem, entered, coef_send, coef_recv, out_send, out_recv,
):
    dev = n_aux * n_lmo
    rows, ao, _ = aux_hbm.shape
    blocks = ao // BLK
    per = lmo_hbm.shape[0]
    lmos = per * dev
    planes = dev // plane
    pitch = half.shape[0] // lmos
    me = lax.axis_index("aux") * n_lmo + lax.axis_index("lmo")
    my_plane, seat = me // plane, lax.rem(me, plane)

    def coords(d):
        return (d // n_lmo, lax.rem(d, n_lmo))

    barrier = pltpu.get_barrier_semaphore()
    before = dev - plane
    in_last = my_plane == planes - 1

    def others(first, last, act):
        @pl.loop(first, last)
        def _(d):
            @pl.when(d != me)
            def _():
                act(d)

    small = [
        pltpu.make_async_copy(src, dst, in_sem.at[n])
        for n, (src, dst) in enumerate((
            (lmo_hbm, lmo_ref), (ao_dom_hbm, ao_dom), (ao_cnt_hbm, ao_cnt),
            (pao_dom_hbm, pao_dom), (pao_cnt_hbm, pao_cnt), (order_hbm, order),
        ))
    ]
    for copy in small:
        copy.start()

    @pl.when(in_last)
    def _():
        for j in range(1, plane):
            d = before + lax.rem(seat + j, plane)
            pl.semaphore_signal(barrier, inc=1, device_id=coords(d), device_id_type=MESH)

    if planes > 1:
        @pl.when(jnp.logical_not(in_last))
        def _():
            for t in range(1, dev):
                d = lax.rem(me + t, dev)
                pl.semaphore_signal(barrier, inc=1, device_id=coords(d), device_id_type=MESH)

    def load(p):
        return pltpu.make_async_copy(aux_hbm.at[p], aux.at[p], aux_sem.at[p])

    for p in range(rows):
        load(p).start()
    pao_load = pltpu.make_async_copy(pao_hbm, pao, pao_sem)
    pao_load.start()

    def coef_copy(slot, d):
        return pltpu.make_async_remote_copy(
            src_ref=lmo_ref, dst_ref=coef_all.at[slot],
            send_sem=coef_send, recv_sem=coef_recv,
            device_id=coords(d), device_id_type=MESH,
        )

    @pl.when(in_last)
    def _():
        pl.semaphore_wait(barrier, dev - 1)

        @pl.loop(0, before)
        def _(d):
            pl.semaphore_signal(entered.at[me], inc=1, device_id=coords(d), device_id_type=MESH)

    if planes > 1:
        @pl.when(jnp.logical_not(in_last))
        def _():
            pl.semaphore_wait(barrier, before - 1)

    small[0].wait()
    for i in range(planes - 2, -1, -1):
        others(i * plane, (i + 1) * plane, lambda d: coef_copy(me, d).start())
    others(before, jnp.where(in_last, dev, before), lambda d: coef_copy(me, d).start())

    coef_all[me] = lmo_ref[...]
    for copy in small[1:]:
        copy.wait()

    eye = lax.broadcasted_iota(jnp.int32, (lmos, lmos), 0) == lax.broadcasted_iota(
        jnp.int32, (lmos, lmos), 1
    )
    where_to = []
    for k in range(DB):
        block = jnp.where(ao_cnt[...] > k, ao_dom[k:k + 1, :], -1).astype(jnp.float32)
        column = jnp.sum(jnp.where(eye, block, 0.0), axis=1, keepdims=True)
        where_to.append(jnp.broadcast_to(column, (lmos, BLK)))

    def turn(p):
        load(p).wait()
        aux_t[p] = aux[p].T

    for p in range(rows // 2):
        turn(p)

    @pl.loop(before, jnp.where(in_last, before, dev))
    def _(d):
        pl.semaphore_wait(entered.at[d], 1)
        coef_copy(me, d).start()

    for p in range(rows // 2, rows):
        turn(p)

    all_coefs = pltpu.make_async_remote_copy(
        src_ref=coef_all.at[pl.ds(0, dev - 1)], dst_ref=coef_all.at[pl.ds(0, dev - 1)],
        send_sem=coef_send, recv_sem=coef_recv,
        device_id=coords(me), device_id_type=MESH,
    )
    all_coefs.wait_recv()

    for d in range(dev):
        coef32[d * per:(d + 1) * per, :] = coef_all[d].astype(jnp.float32)
    for b in range(blocks):
        total = jnp.zeros((lmos, BLK), jnp.float32)
        for k in range(DB):
            total = jnp.where(where_to[k] == b, coef32[:, k * BLK:(k + 1) * BLK], total)
        dense[:, b * BLK:(b + 1) * BLK] = total.astype(jnp.bfloat16)

    wide = 2
    for p in range(rows):
        for b in range(0, blocks, wide):
            out = jnp.dot(
                dense[...], aux_t[p, :, b * BLK:(b + wide) * BLK],
                preferred_element_type=jnp.float32,
            )
            for c in range(wide):
                half[pl.ds((b + c) * rows + p, lmos, stride=pitch), :] = (
                    out[:, c * BLK:(c + 1) * BLK]
                )

    def pack(d, dst):
        lmo = [order[d * per + j] for j in range(per)]
        ends, end = [], jnp.int32(0)
        for j in range(per - 1):
            end = end + pao_cnt[lmo[j]] - 1
            ends.append(end)
        for s in range(USED):
            if s < per:
                i, k = lmo[s], 0
            else:
                i, k = lmo[0], jnp.int32(s - per + 1)
                for j in range(1, per):
                    past = s - per >= ends[j - 1]
                    i = jnp.where(past, lmo[j], i)
                    k = jnp.where(past, s - per + 1 - ends[j - 1], k)
                k = jnp.minimum(k, PB - 1)
            row = i * pitch + pao_dom[k, i] * rows
            dst[s] = half[pl.ds(row, rows), :].astype(jnp.bfloat16)

    def out_copy(slot, d):
        return pltpu.make_async_remote_copy(
            src_ref=send.at[d], dst_ref=recv.at[slot],
            send_sem=out_send, recv_sem=out_recv.at[slot // plane],
            device_id=coords(d), device_id_type=MESH,
        )

    def rows_of(first, count, sem):
        return pltpu.make_async_remote_copy(
            src_ref=send.at[pl.ds(first, count)], dst_ref=recv.at[pl.ds(first, count)],
            send_sem=out_send, recv_sem=sem,
            device_id=coords(me), device_id_type=MESH,
        )

    half_way = planes // 2

    def target(t):
        i, j = t // plane, lax.rem(t, plane)
        down = planes - 1 - i
        other = jnp.where(
            my_plane < half_way,
            jnp.where(down <= my_plane, down - 1, down),
            jnp.where(i >= my_plane, i + 1, i),
        )
        if planes > 2:
            other = jnp.where(in_last, jnp.where(i == 0, planes - 2, i - 1), other)
        return jnp.where(
            i >= planes - 1,
            my_plane * plane + lax.rem(seat + 1 + j, plane),
            other * plane + lax.rem(seat + j, plane),
        )

    pack(target(0), send.at[target(0)])

    @pl.loop(0, dev - 2)
    def _(t):
        pack(target(t + 1), send.at[target(t + 1)])
        out_copy(me, target(t)).start()

    pack(me, recv.at[me])
    out_copy(me, target(dev - 2)).start()

    npao = pao.shape[3]
    pao_load.wait()
    start = jnp.int32(0)
    for g in range(per):
        more = pao_cnt[order[me * per + g]] - 1
        pao_slots[g, :BLK] = pao[g, 0]
        for s in range(USED - per):
            k = s - start
            tile = pao[g, jnp.clip(k + 1, 0, PB - 1)]
            pao_slots[g, (s + 1) * BLK:(s + 2) * BLK] = jnp.where(
                (k >= 0) & (k < more), tile, jnp.zeros_like(tile)
            )
        start = start + more

    def project(n, i):
        first = pl.multiple_of(i * plane, plane)
        own = n == 0
        rows_of(first, plane - own, out_recv.at[i]).wait_recv()
        here = [
            recv[pl.ds(first, plane), s].astype(jnp.float32).reshape(plane * rows, BLK).astype(jnp.bfloat16)
            for s in range(USED)
        ]
        to = pl.multiple_of(i * (plane * rows), plane * rows)
        for g in range(per):
            pair[g, pl.ds(to, plane * rows), :] = jnp.dot(
                jnp.concatenate([here[g]] + here[per:], axis=1), pao_slots[g],
                preferred_element_type=jnp.float32,
            ).astype(jnp.bfloat16)

    last = jnp.where(my_plane < half_way, planes - 1, half_way - 1)
    low, high = jnp.minimum(my_plane, last), jnp.maximum(my_plane, last)
    arrivals = [my_plane]
    for n in range(planes - 2):
        i = planes - 1 - n
        i = jnp.where(i <= high, i - 1, i)
        i = jnp.where(i <= low, i - 1, i)
        arrivals.append(jnp.where(my_plane < half_way, jnp.where(n >= my_plane, n + 1, n), i))
    if planes > 1:
        arrivals.append(last)
    for n, i in enumerate(arrivals):
        project(n, i)
    all_coefs.wait_send()
    rows_of(0, dev - 1, out_recv.at[0]).wait_send()


def contract(pair, pair_out, metric_out, metric, pair_sem, metric_sem):
    per, total, _ = pair.shape
    copies = [pltpu.make_async_copy(pair, pair_out, pair_sem)]
    copies[0].start()
    for g in range(per):
        row = pair[g]
        metric[g] = lax.dot_general(
            row, row, (((0,), (0,)), ((), ())), preferred_element_type=jnp.float32
        ) / total
        copies.append(pltpu.make_async_copy(metric.at[g], metric_out.at[g], metric_sem.at[g]))
        copies[-1].start()
    for copy in copies:
        copy.wait()


def shards(mesh, aux_ints, lmo_coef, ao_domain, ao_count, pao_domain, pao_count, owner_order, pao_coef):
    n_aux, n_lmo = mesh.shape["aux"], mesh.shape["lmo"]
    dev = n_aux * n_lmo
    rows, ao, _ = aux_ints.shape
    blocks = ao // BLK
    per = lmo_coef.shape[0]
    lmos = per * dev
    npao = pao_coef.shape[2]
    across = n_lmo // 2 if n_lmo % 2 == 0 and n_aux % (n_lmo // 2) == 0 else 1
    plane = across * n_lmo
    vmem = pl.BlockSpec(memory_space=pltpu.VMEM)
    anywhere = pl.BlockSpec(memory_space=pl.ANY)
    pair = pl.pallas_call(
        functools.partial(exchange, n_aux, n_lmo, plane),
        out_shape=pltpu.VMEM((per, dev * rows, npao), jnp.bfloat16),
        in_specs=[anywhere] * 8,
        out_specs=vmem,
        scratch_shapes=[
            pltpu.VMEM((rows, ao, ao), jnp.bfloat16),
            pltpu.VMEM((rows, ao, ao), jnp.bfloat16),
            pltpu.VMEM((per, DB * BLK), jnp.bfloat16),
            pltpu.VMEM((DB, lmos), jnp.int32),
            pltpu.VMEM((1, lmos), jnp.int32),
            pltpu.SMEM((PB, lmos), jnp.int32),
            pltpu.SMEM((lmos,), jnp.int32),
            pltpu.SMEM((lmos,), jnp.int32),
            pltpu.VMEM((dev, per, DB * BLK), jnp.bfloat16),
            pltpu.VMEM((lmos, DB * BLK), jnp.float32),
            pltpu.VMEM((lmos, ao), jnp.bfloat16),
            pltpu.VMEM((lmos * (blocks * rows + 4), BLK), jnp.float32),
            pltpu.VMEM((dev, USED, rows, BLK), jnp.bfloat16),
            pltpu.VMEM((dev, USED, rows, BLK), jnp.bfloat16),
            pltpu.VMEM((per, PB, BLK, npao), jnp.bfloat16),
            pltpu.VMEM((per, (USED - per + 1) * BLK, npao), jnp.bfloat16),
            pltpu.SemaphoreType.DMA((rows,)),
            pltpu.SemaphoreType.DMA((6,)),
            pltpu.SemaphoreType.DMA,
            pltpu.SemaphoreType.REGULAR((dev,)),
            pltpu.SemaphoreType.DMA,
            pltpu.SemaphoreType.DMA,
            pltpu.SemaphoreType.DMA,
            pltpu.SemaphoreType.DMA((dev // plane,)),
        ],
        compiler_params=pltpu.CompilerParams(
            collective_id=0, has_side_effects=True, vmem_limit_bytes=48 * 2**20
        ),
        name="exchange",
    )(*(
        pltpu.with_memory_space_constraint(x, pltpu.HBM)
        for x in (
            aux_ints, lmo_coef, ao_domain.T, ao_count.reshape(1, lmos), pao_domain.T, pao_count,
            owner_order, pao_coef.reshape(per, PB, BLK, npao),
        )
    ))
    return pl.pallas_call(
        contract,
        out_shape=(
            jax.ShapeDtypeStruct((per, dev * rows, npao), jnp.bfloat16),
            jax.ShapeDtypeStruct((per, npao, npao), jnp.float32),
        ),
        in_specs=[vmem],
        out_specs=(anywhere, anywhere),
        scratch_shapes=[
            pltpu.VMEM((per, npao, npao), jnp.float32),
            pltpu.SemaphoreType.DMA,
            pltpu.SemaphoreType.DMA((per,)),
        ],
        compiler_params=pltpu.CompilerParams(vmem_limit_bytes=16 * 2**20),
        name="contract",
    )(pair)


def solution(mesh):
    split = ("aux", "lmo")
    placed = (P(split, None, None), P(split, None), P(), P(), P(), P(), P(), P(split, None, None))
    return jax.shard_map(
        functools.partial(shards, mesh),
        mesh=mesh,
        in_specs=placed,
        out_specs=(P(split, None, None), P(split, None, None)),
        check_vma=False,
    )
```

```python
import functools

import jax
import jax.numpy as jnp
from jax import lax
from jax.experimental import pallas as pl
from jax.experimental.pallas import tpu as pltpu
from jax.sharding import PartitionSpec as P

BLK = 128
DB = 3
PB = 3
USED = 8
PARTS = 2
EARLY = 8
MESH = pl.DeviceIdType.MESH


def exchange(
    n_aux, n_lmo, plane,
    aux_hbm, lmo_hbm, ao_dom_hbm, ao_cnt_hbm, pao_dom_hbm, pao_cnt_hbm, order_hbm, pao_hbm, pair,
    aux, aux_t, lmo_ref, ao_dom, ao_cnt, pao_dom, pao_cnt, order,
    coef_all, coef32, dense, half, send, recv, pao, pao_slots,
    aux_sem, in_sem, pao_sem, entered, coef_send, coef_recv, out_send, out_recv,
):
    dev = n_aux * n_lmo
    rows, ao, _ = aux_hbm.shape
    blocks = ao // BLK
    per = lmo_hbm.shape[0]
    lmos = per * dev
    planes = dev // plane
    pitch = half.shape[0] // lmos
    me = lax.axis_index("aux") * n_lmo + lax.axis_index("lmo")
    my_plane, seat = me // plane, lax.rem(me, plane)

    def coords(d):
        return (d // n_lmo, lax.rem(d, n_lmo))

    barrier = pltpu.get_barrier_semaphore()
    before = dev - plane
    in_last = my_plane == planes - 1

    def others(first, last, act):
        @pl.loop(first, last)
        def _(d):
            @pl.when(d != me)
            def _():
                act(d)

    small = [
        pltpu.make_async_copy(src, dst, in_sem.at[n])
        for n, (src, dst) in enumerate((
            (lmo_hbm, lmo_ref), (ao_dom_hbm, ao_dom), (ao_cnt_hbm, ao_cnt),
            (pao_dom_hbm, pao_dom), (pao_cnt_hbm, pao_cnt), (order_hbm, order),
        ))
    ]
    for copy in small:
        copy.start()

    @pl.when(in_last)
    def _():
        for j in range(1, plane):
            d = before + lax.rem(seat + j, plane)
            pl.semaphore_signal(barrier, inc=1, device_id=coords(d), device_id_type=MESH)

    if planes > 1:
        @pl.when(jnp.logical_not(in_last))
        def _():
            for t in range(1, dev):
                d = lax.rem(me + t, dev)
                pl.semaphore_signal(barrier, inc=1, device_id=coords(d), device_id_type=MESH)

    def load(p):
        return pltpu.make_async_copy(aux_hbm.at[p], aux.at[p], aux_sem.at[p])

    for p in range(rows):
        load(p).start()
    pao_load = pltpu.make_async_copy(pao_hbm, pao, pao_sem)
    pao_load.start()

    def coef_copy(slot, d):
        return pltpu.make_async_remote_copy(
            src_ref=lmo_ref, dst_ref=coef_all.at[slot],
            send_sem=coef_send, recv_sem=coef_recv,
            device_id=coords(d), device_id_type=MESH,
        )

    @pl.when(in_last)
    def _():
        pl.semaphore_wait(barrier, dev - 1)

        @pl.loop(0, before)
        def _(d):
            pl.semaphore_signal(entered.at[me], inc=1, device_id=coords(d), device_id_type=MESH)

    if planes > 1:
        @pl.when(jnp.logical_not(in_last))
        def _():
            pl.semaphore_wait(barrier, before - 1)

    small[0].wait()
    for i in range(planes - 2, -1, -1):
        others(i * plane, (i + 1) * plane, lambda d: coef_copy(me, d).start())
    others(before, jnp.where(in_last, dev, before), lambda d: coef_copy(me, d).start())

    coef_all[me] = lmo_ref[...]
    for copy in small[1:]:
        copy.wait()

    eye = lax.broadcasted_iota(jnp.int32, (lmos, lmos), 0) == lax.broadcasted_iota(
        jnp.int32, (lmos, lmos), 1
    )
    where_to = []
    for k in range(DB):
        block = jnp.where(ao_cnt[...] > k, ao_dom[k:k + 1, :], -1).astype(jnp.float32)
        column = jnp.sum(jnp.where(eye, block, 0.0), axis=1, keepdims=True)
        where_to.append(jnp.broadcast_to(column, (lmos, BLK)))

    def turn(p):
        load(p).wait()
        aux_t[p] = aux[p].T

    for p in range(rows // 2):
        turn(p)

    @pl.loop(before, jnp.where(in_last, before, dev))
    def _(d):
        pl.semaphore_wait(entered.at[d], 1)
        coef_copy(me, d).start()

    for p in range(rows // 2, rows):
        turn(p)

    all_coefs = pltpu.make_async_remote_copy(
        src_ref=coef_all.at[pl.ds(0, dev - 1)], dst_ref=coef_all.at[pl.ds(0, dev - 1)],
        send_sem=coef_send, recv_sem=coef_recv,
        device_id=coords(me), device_id_type=MESH,
    )
    all_coefs.wait_recv()

    for d in range(dev):
        coef32[d * per:(d + 1) * per, :] = coef_all[d].astype(jnp.float32)
    for b in range(blocks):
        total = jnp.zeros((lmos, BLK), jnp.float32)
        for k in range(DB):
            total = jnp.where(where_to[k] == b, coef32[:, k * BLK:(k + 1) * BLK], total)
        dense[:, b * BLK:(b + 1) * BLK] = total.astype(jnp.bfloat16)

    part = rows // PARTS

    def pack(d, dst, parts):
        lmo = [order[d * per + j] for j in range(per)]
        ends, end = [], jnp.int32(0)
        for j in range(per - 1):
            end = end + pao_cnt[lmo[j]] - 1
            ends.append(end)
        for s in range(USED):
            if s < per:
                i, k = lmo[s], 0
            else:
                i, k = lmo[0], jnp.int32(s - per + 1)
                for j in range(1, per):
                    past = s - per >= ends[j - 1]
                    i = jnp.where(past, lmo[j], i)
                    k = jnp.where(past, s - per + 1 - ends[j - 1], k)
                k = jnp.minimum(k, PB - 1)
            row = i * pitch + pao_dom[k, i] * rows
            for h in parts:
                dst[h, s] = half[pl.ds(row + h * part, part), :].astype(jnp.bfloat16)

    def out_copy(slot, d, h=None):
        return pltpu.make_async_remote_copy(
            src_ref=send.at[d] if h is None else send.at[d, h],
            dst_ref=recv.at[slot] if h is None else recv.at[slot, h],
            send_sem=out_send, recv_sem=out_recv.at[slot // plane],
            device_id=coords(d), device_id_type=MESH,
        )

    def rows_of(first, count, sem):
        return pltpu.make_async_remote_copy(
            src_ref=send.at[pl.ds(first, count)], dst_ref=recv.at[pl.ds(first, count)],
            send_sem=out_send, recv_sem=sem,
            device_id=coords(me), device_id_type=MESH,
        )

    half_way = planes // 2

    def target(t):
        i, j = t // plane, lax.rem(t, plane)
        rest = i - (planes - half_way)
        other = jnp.where(
            my_plane < half_way,
            jnp.where(rest < 0, i + half_way, jnp.where(rest >= my_plane, rest + 1, rest)),
            jnp.where(i >= my_plane, i + 1, i),
        )
        return jnp.where(
            i >= planes - 1,
            my_plane * plane + lax.rem(seat + 1 + j, plane),
            other * plane + lax.rem(seat + j, plane),
        )

    wide = 2

    def transform(p):
        for b in range(0, blocks, wide):
            out = jnp.dot(
                dense[...], aux_t[p, :, b * BLK:(b + wide) * BLK],
                preferred_element_type=jnp.float32,
            )
            for c in range(wide):
                half[pl.ds((b + c) * rows + p, lmos, stride=pitch), :] = (
                    out[:, c * BLK:(c + 1) * BLK]
                )

    held = None
    for h in range(PARTS):
        for p in range(h * part, (h + 1) * part):
            transform(p)
            if held is not None:
                held.start()
                held = None
        for t in range(EARLY):
            d = target(t)
            pack(d, send.at[d], (h,))
            if held is not None:
                held.start()
            held = out_copy(me, d, h)
    pack(target(EARLY), send.at[target(EARLY)], range(PARTS))
    held.start()

    @pl.loop(EARLY, dev - 2)
    def _(t):
        pack(target(t + 1), send.at[target(t + 1)], range(PARTS))
        out_copy(me, target(t)).start()

    pack(me, recv.at[me], range(PARTS))
    out_copy(me, target(dev - 2)).start()

    npao = pao.shape[3]
    pao_load.wait()
    start = jnp.int32(0)
    for g in range(per):
        more = pao_cnt[order[me * per + g]] - 1
        pao_slots[g, :BLK] = pao[g, 0]
        for s in range(USED - per):
            k = s - start
            tile = pao[g, jnp.clip(k + 1, 0, PB - 1)]
            pao_slots[g, (s + 1) * BLK:(s + 2) * BLK] = jnp.where(
                (k >= 0) & (k < more), tile, jnp.zeros_like(tile)
            )
        start = start + more

    def project(n, i):
        first = pl.multiple_of(i * plane, plane)
        own = n == 0
        rows_of(first, plane - own, out_recv.at[i]).wait_recv()
        here = [
            jnp.concatenate(
                [recv[pl.ds(first, plane), h, s].astype(jnp.float32) for h in range(PARTS)], axis=1
            ).reshape(plane * rows, BLK).astype(jnp.bfloat16)
            for s in range(USED)
        ]
        to = pl.multiple_of(i * (plane * rows), plane * rows)
        for g in range(per):
            pair[g, pl.ds(to, plane * rows), :] = jnp.dot(
                jnp.concatenate([here[g]] + here[per:], axis=1), pao_slots[g],
                preferred_element_type=jnp.float32,
            ).astype(jnp.bfloat16)

    last = jnp.where(in_last, half_way - 1, my_plane + 1)
    low, high = jnp.minimum(my_plane, last), jnp.maximum(my_plane, last)
    arrivals = [my_plane]
    for n in range(planes - 2):
        i = planes - 1 - n
        i = jnp.where(i <= high, i - 1, i)
        i = jnp.where(i <= low, i - 1, i)
        arrivals.append(i)
    if planes > 1:
        arrivals.append(last)
    for n, i in enumerate(arrivals):
        project(n, i)
    all_coefs.wait_send()
    rows_of(0, dev - 1, out_recv.at[0]).wait_send()


def contract(pair, pair_out, metric_out, metric, pair_sem, metric_sem):
    per, total, _ = pair.shape
    copies = [pltpu.make_async_copy(pair, pair_out, pair_sem)]
    copies[0].start()
    for g in range(per):
        row = pair[g]
        metric[g] = lax.dot_general(
            row, row, (((0,), (0,)), ((), ())), preferred_element_type=jnp.float32
        ) / total
        copies.append(pltpu.make_async_copy(metric.at[g], metric_out.at[g], metric_sem.at[g]))
        copies[-1].start()
    for copy in copies:
        copy.wait()


def shards(mesh, aux_ints, lmo_coef, ao_domain, ao_count, pao_domain, pao_count, owner_order, pao_coef):
    n_aux, n_lmo = mesh.shape["aux"], mesh.shape["lmo"]
    dev = n_aux * n_lmo
    rows, ao, _ = aux_ints.shape
    blocks = ao // BLK
    per = lmo_coef.shape[0]
    lmos = per * dev
    npao = pao_coef.shape[2]
    across = n_lmo // 2 if n_lmo % 2 == 0 and n_aux % (n_lmo // 2) == 0 else 1
    plane = across * n_lmo
    vmem = pl.BlockSpec(memory_space=pltpu.VMEM)
    anywhere = pl.BlockSpec(memory_space=pl.ANY)
    pair = pl.pallas_call(
        functools.partial(exchange, n_aux, n_lmo, plane),
        out_shape=pltpu.VMEM((per, dev * rows, npao), jnp.bfloat16),
        in_specs=[anywhere] * 8,
        out_specs=vmem,
        scratch_shapes=[
            pltpu.VMEM((rows, ao, ao), jnp.bfloat16),
            pltpu.VMEM((rows, ao, ao), jnp.bfloat16),
            pltpu.VMEM((per, DB * BLK), jnp.bfloat16),
            pltpu.VMEM((DB, lmos), jnp.int32),
            pltpu.VMEM((1, lmos), jnp.int32),
            pltpu.SMEM((PB, lmos), jnp.int32),
            pltpu.SMEM((lmos,), jnp.int32),
            pltpu.SMEM((lmos,), jnp.int32),
            pltpu.VMEM((dev, per, DB * BLK), jnp.bfloat16),
            pltpu.VMEM((lmos, DB * BLK), jnp.float32),
            pltpu.VMEM((lmos, ao), jnp.bfloat16),
            pltpu.VMEM((lmos * (blocks * rows + 4), BLK), jnp.float32),
            pltpu.VMEM((dev, PARTS, USED, rows // PARTS, BLK), jnp.bfloat16),
            pltpu.VMEM((dev, PARTS, USED, rows // PARTS, BLK), jnp.bfloat16),
            pltpu.VMEM((per, PB, BLK, npao), jnp.bfloat16),
            pltpu.VMEM((per, (USED - per + 1) * BLK, npao), jnp.bfloat16),
            pltpu.SemaphoreType.DMA((rows,)),
            pltpu.SemaphoreType.DMA((6,)),
            pltpu.SemaphoreType.DMA,
            pltpu.SemaphoreType.REGULAR((dev,)),
            pltpu.SemaphoreType.DMA,
            pltpu.SemaphoreType.DMA,
            pltpu.SemaphoreType.DMA,
            pltpu.SemaphoreType.DMA((dev // plane,)),
        ],
        compiler_params=pltpu.CompilerParams(
            collective_id=0, has_side_effects=True, vmem_limit_bytes=48 * 2**20
        ),
        name="exchange",
    )(*(
        pltpu.with_memory_space_constraint(x, pltpu.HBM)
        for x in (
            aux_ints, lmo_coef, ao_domain.T, ao_count.reshape(1, lmos), pao_domain.T, pao_count,
            owner_order, pao_coef.reshape(per, PB, BLK, npao),
        )
    ))
    return pl.pallas_call(
        contract,
        out_shape=(
            jax.ShapeDtypeStruct((per, dev * rows, npao), jnp.bfloat16),
            jax.ShapeDtypeStruct((per, npao, npao), jnp.float32),
        ),
        in_specs=[vmem],
        out_specs=(anywhere, anywhere),
        scratch_shapes=[
            pltpu.VMEM((per, npao, npao), jnp.float32),
            pltpu.SemaphoreType.DMA,
            pltpu.SemaphoreType.DMA((per,)),
        ],
        compiler_params=pltpu.CompilerParams(vmem_limit_bytes=16 * 2**20),
        name="contract",
    )(pair)


def solution(mesh):
    split = ("aux", "lmo")
    placed = (P(split, None, None), P(split, None), P(), P(), P(), P(), P(), P(split, None, None))
    return jax.shard_map(
        functools.partial(shards, mesh),
        mesh=mesh,
        in_specs=placed,
        out_specs=(P(split, None, None), P(split, None, None)),
        check_vma=False,
    )
```

```python
import functools

import jax
import jax.numpy as jnp
from jax import lax
from jax.experimental import pallas as pl
from jax.experimental.pallas import tpu as pltpu
from jax.sharding import PartitionSpec as P

BLK = 128
DB = 3
PB = 3
USED = 8
PARTS = 2
EARLY = 6
MESH = pl.DeviceIdType.MESH


def exchange(
    n_aux, n_lmo, plane,
    aux_hbm, lmo_hbm, ao_dom_hbm, ao_cnt_hbm, pao_dom_hbm, pao_cnt_hbm, order_hbm, pao_hbm, pair,
    aux, aux_t, lmo_ref, ao_dom, ao_cnt, pao_dom, pao_cnt, order,
    coef_all, coef32, dense, half, tab, send, recv, pao, pao_slots,
    aux_sem, in_sem, pao_sem, entered, coef_send, coef_recv, out_send, out_recv,
):
    dev = n_aux * n_lmo
    rows, ao, _ = aux_hbm.shape
    blocks = ao // BLK
    per = lmo_hbm.shape[0]
    lmos = per * dev
    planes = dev // plane
    pitch = half.shape[0] // lmos
    me = lax.axis_index("aux") * n_lmo + lax.axis_index("lmo")
    my_plane, seat = me // plane, lax.rem(me, plane)

    def coords(d):
        return (d // n_lmo, lax.rem(d, n_lmo))

    barrier = pltpu.get_barrier_semaphore()
    before = dev - plane
    in_last = my_plane == planes - 1

    def others(first, last, act):
        @pl.loop(first, last)
        def _(d):
            @pl.when(d != me)
            def _():
                act(d)

    small = [
        pltpu.make_async_copy(src, dst, in_sem.at[n])
        for n, (src, dst) in enumerate((
            (lmo_hbm, lmo_ref), (ao_dom_hbm, ao_dom), (ao_cnt_hbm, ao_cnt),
            (pao_dom_hbm, pao_dom), (pao_cnt_hbm, pao_cnt), (order_hbm, order),
        ))
    ]
    for copy in small:
        copy.start()

    @pl.when(in_last)
    def _():
        for j in range(1, plane):
            d = before + lax.rem(seat + j, plane)
            pl.semaphore_signal(barrier, inc=1, device_id=coords(d), device_id_type=MESH)

    if planes > 1:
        @pl.when(jnp.logical_not(in_last))
        def _():
            for t in range(1, dev):
                d = lax.rem(me + t, dev)
                pl.semaphore_signal(barrier, inc=1, device_id=coords(d), device_id_type=MESH)

    def load(p):
        return pltpu.make_async_copy(aux_hbm.at[p], aux.at[p], aux_sem.at[p])

    for p in range(rows):
        load(p).start()
    pao_load = pltpu.make_async_copy(pao_hbm, pao, pao_sem)
    pao_load.start()

    def coef_copy(slot, d):
        return pltpu.make_async_remote_copy(
            src_ref=lmo_ref, dst_ref=coef_all.at[slot],
            send_sem=coef_send, recv_sem=coef_recv,
            device_id=coords(d), device_id_type=MESH,
        )

    @pl.when(in_last)
    def _():
        pl.semaphore_wait(barrier, dev - 1)

        @pl.loop(0, before)
        def _(d):
            pl.semaphore_signal(entered.at[me], inc=1, device_id=coords(d), device_id_type=MESH)

    if planes > 1:
        @pl.when(jnp.logical_not(in_last))
        def _():
            pl.semaphore_wait(barrier, before - 1)

    small[0].wait()
    for i in range(planes - 2, -1, -1):
        others(i * plane, (i + 1) * plane, lambda d: coef_copy(me, d).start())
    others(before, jnp.where(in_last, dev, before), lambda d: coef_copy(me, d).start())

    coef_all[me] = lmo_ref[...]
    for copy in small[1:]:
        copy.wait()

    eye = lax.broadcasted_iota(jnp.int32, (lmos, lmos), 0) == lax.broadcasted_iota(
        jnp.int32, (lmos, lmos), 1
    )
    where_to = []
    for k in range(DB):
        block = jnp.where(ao_cnt[...] > k, ao_dom[k:k + 1, :], -1).astype(jnp.float32)
        column = jnp.sum(jnp.where(eye, block, 0.0), axis=1, keepdims=True)
        where_to.append(jnp.broadcast_to(column, (lmos, BLK)))

    half_way = planes // 2

    def target(t):
        i, j = t // plane, lax.rem(t, plane)
        rest = i - (planes - half_way)
        other = jnp.where(
            my_plane < half_way,
            jnp.where(rest < 0, i + half_way, jnp.where(rest >= my_plane, rest + 1, rest)),
            jnp.where(i >= my_plane, i + 1, i),
        )
        return jnp.where(
            i >= planes - 1,
            my_plane * plane + lax.rem(seat + 1 + j, plane),
            other * plane + lax.rem(seat + j, plane),
        )

    def slot_rows(d):
        lmo = [order[d * per + j] for j in range(per)]
        ends, end = [], jnp.int32(0)
        for j in range(per - 1):
            end = end + pao_cnt[lmo[j]] - 1
            ends.append(end)
        found = []
        for s in range(USED):
            if s < per:
                i, k = lmo[s], 0
            else:
                i, k = lmo[0], jnp.int32(s - per + 1)
                for j in range(1, per):
                    past = s - per >= ends[j - 1]
                    i = jnp.where(past, lmo[j], i)
                    k = jnp.where(past, s - per + 1 - ends[j - 1], k)
                k = jnp.minimum(k, PB - 1)
            found.append(i * pitch + pao_dom[k, i] * rows)
        return found

    def turn(p):
        load(p).wait()
        aux_t[p] = aux[p].T
        for t in range(p * EARLY // rows, (p + 1) * EARLY // rows):
            for s, row in enumerate(slot_rows(target(t))):
                tab[t * USED + s] = row

    for p in range(rows // 2):
        turn(p)

    @pl.loop(before, jnp.where(in_last, before, dev))
    def _(d):
        pl.semaphore_wait(entered.at[d], 1)
        coef_copy(me, d).start()

    for p in range(rows // 2, rows):
        turn(p)

    all_coefs = pltpu.make_async_remote_copy(
        src_ref=coef_all.at[pl.ds(0, dev - 1)], dst_ref=coef_all.at[pl.ds(0, dev - 1)],
        send_sem=coef_send, recv_sem=coef_recv,
        device_id=coords(me), device_id_type=MESH,
    )
    all_coefs.wait_recv()

    for d in range(dev):
        coef32[d * per:(d + 1) * per, :] = coef_all[d].astype(jnp.float32)
    for b in range(blocks):
        total = jnp.zeros((lmos, BLK), jnp.float32)
        for k in range(DB):
            total = jnp.where(where_to[k] == b, coef32[:, k * BLK:(k + 1) * BLK], total)
        dense[:, b * BLK:(b + 1) * BLK] = total.astype(jnp.bfloat16)

    part = rows // PARTS

    def pack(d, dst, parts, found=None):
        for s, row in enumerate(found if found else slot_rows(d)):
            for h in parts:
                dst[h, s] = half[pl.ds(row + h * part, part), :].astype(jnp.bfloat16)

    def out_copy(slot, d, h=None):
        return pltpu.make_async_remote_copy(
            src_ref=send.at[d] if h is None else send.at[d, h],
            dst_ref=recv.at[slot] if h is None else recv.at[slot, h],
            send_sem=out_send, recv_sem=out_recv.at[slot // plane],
            device_id=coords(d), device_id_type=MESH,
        )

    def rows_of(first, count, sem):
        return pltpu.make_async_remote_copy(
            src_ref=send.at[pl.ds(first, count)], dst_ref=recv.at[pl.ds(first, count)],
            send_sem=out_send, recv_sem=sem,
            device_id=coords(me), device_id_type=MESH,
        )

    wide = 2

    def transform(p):
        for b in range(0, blocks, wide):
            out = jnp.dot(
                dense[...], aux_t[p, :, b * BLK:(b + wide) * BLK],
                preferred_element_type=jnp.float32,
            )
            for c in range(wide):
                half[pl.ds((b + c) * rows + p, lmos, stride=pitch), :] = (
                    out[:, c * BLK:(c + 1) * BLK]
                )

    held = None
    for h in range(PARTS):
        for p in range(h * part, (h + 1) * part):
            transform(p)
            if held is not None:
                held.start()
                held = None
        for t in range(EARLY):
            d = target(t)
            pack(d, send.at[d], (h,), [tab[t * USED + s] for s in range(USED)])
            if held is not None:
                held.start()
            held = out_copy(me, d, h)
    pack(target(EARLY), send.at[target(EARLY)], range(PARTS))
    held.start()

    @pl.loop(EARLY, dev - 2)
    def _(t):
        pack(target(t + 1), send.at[target(t + 1)], range(PARTS))
        out_copy(me, target(t)).start()

    pack(me, recv.at[me], range(PARTS))
    out_copy(me, target(dev - 2)).start()

    npao = pao.shape[3]
    pao_load.wait()
    start = jnp.int32(0)
    for g in range(per):
        more = pao_cnt[order[me * per + g]] - 1
        pao_slots[g, :BLK] = pao[g, 0]
        for s in range(USED - per):
            k = s - start
            tile = pao[g, jnp.clip(k + 1, 0, PB - 1)]
            pao_slots[g, (s + 1) * BLK:(s + 2) * BLK] = jnp.where(
                (k >= 0) & (k < more), tile, jnp.zeros_like(tile)
            )
        start = start + more

    def project(n, i):
        first = pl.multiple_of(i * plane, plane)
        own = n == 0
        rows_of(first, plane - own, out_recv.at[i]).wait_recv()
        here = [
            jnp.concatenate(
                [recv[pl.ds(first, plane), h, s].astype(jnp.float32) for h in range(PARTS)], axis=1
            ).reshape(plane * rows, BLK).astype(jnp.bfloat16)
            for s in range(USED)
        ]
        to = pl.multiple_of(i * (plane * rows), plane * rows)
        for g in range(per):
            pair[g, pl.ds(to, plane * rows), :] = jnp.dot(
                jnp.concatenate([here[g]] + here[per:], axis=1), pao_slots[g],
                preferred_element_type=jnp.float32,
            ).astype(jnp.bfloat16)

    last = jnp.where(in_last, half_way - 1, my_plane + 1)
    low, high = jnp.minimum(my_plane, last), jnp.maximum(my_plane, last)
    arrivals = [my_plane]
    for n in range(planes - 2):
        i = planes - 1 - n
        i = jnp.where(i <= high, i - 1, i)
        i = jnp.where(i <= low, i - 1, i)
        arrivals.append(i)
    if planes > 1:
        arrivals.append(last)
    for n, i in enumerate(arrivals):
        project(n, i)
    all_coefs.wait_send()
    rows_of(0, dev - 1, out_recv.at[0]).wait_send()


def contract(pair, pair_out, metric_out, metric, pair_sem, metric_sem):
    per, total, _ = pair.shape
    copies = [pltpu.make_async_copy(pair, pair_out, pair_sem)]
    copies[0].start()
    for g in range(per):
        row = pair[g]
        metric[g] = lax.dot_general(
            row, row, (((0,), (0,)), ((), ())), preferred_element_type=jnp.float32
        ) / total
        copies.append(pltpu.make_async_copy(metric.at[g], metric_out.at[g], metric_sem.at[g]))
        copies[-1].start()
    for copy in copies:
        copy.wait()


def shards(mesh, aux_ints, lmo_coef, ao_domain, ao_count, pao_domain, pao_count, owner_order, pao_coef):
    n_aux, n_lmo = mesh.shape["aux"], mesh.shape["lmo"]
    dev = n_aux * n_lmo
    rows, ao, _ = aux_ints.shape
    blocks = ao // BLK
    per = lmo_coef.shape[0]
    lmos = per * dev
    npao = pao_coef.shape[2]
    across = n_lmo // 2 if n_lmo % 2 == 0 and n_aux % (n_lmo // 2) == 0 else 1
    plane = across * n_lmo
    vmem = pl.BlockSpec(memory_space=pltpu.VMEM)
    anywhere = pl.BlockSpec(memory_space=pl.ANY)
    pair = pl.pallas_call(
        functools.partial(exchange, n_aux, n_lmo, plane),
        out_shape=pltpu.VMEM((per, dev * rows, npao), jnp.bfloat16),
        in_specs=[anywhere] * 8,
        out_specs=vmem,
        scratch_shapes=[
            pltpu.VMEM((rows, ao, ao), jnp.bfloat16),
            pltpu.VMEM((rows, ao, ao), jnp.bfloat16),
            pltpu.VMEM((per, DB * BLK), jnp.bfloat16),
            pltpu.VMEM((DB, lmos), jnp.int32),
            pltpu.VMEM((1, lmos), jnp.int32),
            pltpu.SMEM((PB, lmos), jnp.int32),
            pltpu.SMEM((lmos,), jnp.int32),
            pltpu.SMEM((lmos,), jnp.int32),
            pltpu.VMEM((dev, per, DB * BLK), jnp.bfloat16),
            pltpu.VMEM((lmos, DB * BLK), jnp.float32),
            pltpu.VMEM((lmos, ao), jnp.bfloat16),
            pltpu.VMEM((lmos * (blocks * rows + 4), BLK), jnp.float32),
            pltpu.SMEM((EARLY * USED,), jnp.int32),
            pltpu.VMEM((dev, PARTS, USED, rows // PARTS, BLK), jnp.bfloat16),
            pltpu.VMEM((dev, PARTS, USED, rows // PARTS, BLK), jnp.bfloat16),
            pltpu.VMEM((per, PB, BLK, npao), jnp.bfloat16),
            pltpu.VMEM((per, (USED - per + 1) * BLK, npao), jnp.bfloat16),
            pltpu.SemaphoreType.DMA((rows,)),
            pltpu.SemaphoreType.DMA((6,)),
            pltpu.SemaphoreType.DMA,
            pltpu.SemaphoreType.REGULAR((dev,)),
            pltpu.SemaphoreType.DMA,
            pltpu.SemaphoreType.DMA,
            pltpu.SemaphoreType.DMA,
            pltpu.SemaphoreType.DMA((dev // plane,)),
        ],
        compiler_params=pltpu.CompilerParams(
            collective_id=0, has_side_effects=True, vmem_limit_bytes=48 * 2**20
        ),
        name="exchange",
    )(*(
        pltpu.with_memory_space_constraint(x, pltpu.HBM)
        for x in (
            aux_ints, lmo_coef, ao_domain.T, ao_count.reshape(1, lmos), pao_domain.T, pao_count,
            owner_order, pao_coef.reshape(per, PB, BLK, npao),
        )
    ))
    return pl.pallas_call(
        contract,
        out_shape=(
            jax.ShapeDtypeStruct((per, dev * rows, npao), jnp.bfloat16),
            jax.ShapeDtypeStruct((per, npao, npao), jnp.float32),
        ),
        in_specs=[vmem],
        out_specs=(anywhere, anywhere),
        scratch_shapes=[
            pltpu.VMEM((per, npao, npao), jnp.float32),
            pltpu.SemaphoreType.DMA,
            pltpu.SemaphoreType.DMA((per,)),
        ],
        compiler_params=pltpu.CompilerParams(vmem_limit_bytes=16 * 2**20),
        name="contract",
    )(pair)


def solution(mesh):
    split = ("aux", "lmo")
    placed = (P(split, None, None), P(split, None), P(), P(), P(), P(), P(), P(split, None, None))
    return jax.shard_map(
        functools.partial(shards, mesh),
        mesh=mesh,
        in_specs=placed,
        out_specs=(P(split, None, None), P(split, None, None)),
        check_vma=False,
    )
```
